128 devices in a mesh: rep: 2 (over core), dp: 64 (over x, y, z).
Axes of the slice: x: 4, y: 4, z: 4, core: 2. Of those that a mesh axis runs over, the one named last changes fastest.
Arguments:
- g_w_gate: bfloat16 [128, 2, 896, 2560], P(('rep', 'dp')), parts along dimension 0
- g_w_up: bfloat16 [128, 2, 896, 2560], P(('rep', 'dp')), parts along dimension 0
- g_w_down: bfloat16 [128, 2, 2560, 896], P(('rep', 'dp')), parts along dimension 0
- w_gate: bfloat16 [2, 896, 2560], replicated
- w_up: bfloat16 [2, 896, 2560], replicated
- w_down: bfloat16 [2, 2560, 896], replicated
- m_w_gate: float32 [2, 896, 2560], P(None, 'dp')
- m_w_up: float32 [2, 896, 2560], P(None, 'dp')
- m_w_down: float32 [2, 2560, 896], P(None, 'dp')
- v_w_gate: float32 [2, 896, 2560], P(None, 'dp')
- v_w_up: float32 [2, 896, 2560], P(None, 'dp')
- v_w_down: float32 [2, 2560, 896], P(None, 'dp')
Outputs:
- output 1: bfloat16 [4, 896, 2560], P('rep'), parts along dimension 0
- output 2: bfloat16 [4, 896, 2560], P('rep'), parts along dimension 0
- output 3: bfloat16 [4, 2560, 896], P('rep'), parts along dimension 0
- output 4: float32 [4, 896, 2560], P('rep', 'dp'), parts along dimension 0
- output 5: float32 [4, 896, 2560], P('rep', 'dp'), parts along dimension 0
- output 6: float32 [4, 2560, 896], P('rep', 'dp'), parts along dimension 0
- output 7: float32 [4, 896, 2560], P('rep', 'dp'), parts along dimension 0
- output 8: float32 [4, 896, 2560], P('rep', 'dp'), parts along dimension 0
- output 9: float32 [4, 2560, 896], P('rep', 'dp'), parts along dimension 0
There are 2 independent parts. The reference program is written for one: setup_inputs(seed, part) draws one part's arguments, and reference() takes and returns one part's arrays. A program takes and returns all parts, laid end to end along the dimension named above; an argument that names none is the same for every part.
All inputs are finite; a program needn't handle non-finite values.
Results may differ from the reference program's by a relative error of at most 0.022.
Values are sent between devices in bfloat16 or wider.
A program may use at most 1.5 GiB of HBM per device.

```python
import jax
import jax.numpy as jnp
from jax import lax

DEVICES = 64
D = 896
FF = 2560
LAYERS = 2
NAMES = ("w_gate", "w_up", "w_down")
SHAPES = {"w_gate": (LAYERS, D, FF), "w_up": (LAYERS, D, FF), "w_down": (LAYERS, FF, D)}


def setup_inputs(seed: int = 0, part: int = 0) -> dict:
    kz, *keys = jax.random.split(jax.random.key(seed), 1 + 5 * len(NAMES))
    loud = 2.0 ** jax.random.uniform(kz, (), jnp.float32, -1.0, 1.0)
    drawn = {}
    for name, key, both in zip(NAMES, keys[:3], keys[3:6], strict=True):
        own = jax.random.normal(jax.random.fold_in(key, part), (DEVICES, *SHAPES[name]), jnp.float32)
        shared = jax.random.normal(jax.random.fold_in(both, part), SHAPES[name], jnp.float32)
        drawn["g_" + name] = (loud * (0.7 * shared / DEVICES + 0.7 * own * DEVICES**-0.5)).astype(jnp.bfloat16)
    for name, key in zip(NAMES, keys[6:9], strict=True):
        drawn[name] = (jax.random.normal(key, SHAPES[name], jnp.float32) * SHAPES[name][1] ** -0.5).astype(jnp.bfloat16)
    for name, key in zip(NAMES, keys[9:12], strict=True):
        drawn["m_" + name] = loud * 0.5 * jax.random.normal(key, SHAPES[name], jnp.float32)
    for name, key in zip(NAMES, keys[12:15], strict=True):
        drawn["v_" + name] = loud * loud * jax.random.uniform(key, SHAPES[name], jnp.float32, 0.5, 1.5)
    return drawn


def adamw(w, m, v, g):
    m = 0.9 * m + 0.1 * g
    v = 0.95 * v + 0.05 * g * g
    step = m * lax.rsqrt(v + 1e-8) + 0.1 * w
    return (w - 0.02 * step).astype(jnp.bfloat16), m, v


def clipped(gradients, sum_of_squares, count):
    factor = jnp.minimum(1.0, 0.5 * lax.rsqrt(sum_of_squares / count + 1e-30))
    return [g * factor for g in gradients]


def reference(g_w_gate, g_w_up, g_w_down, w_gate, w_up, w_down, m_w_gate, m_w_up, m_w_down, v_w_gate, v_w_up, v_w_down):
    def total(terms):
        return lax.scan(lambda so_far, term: (so_far + term.astype(jnp.float32), None), jnp.zeros(terms.shape[1:], jnp.float32), terms)[0]

    gradients = [total(terms).astype(jnp.bfloat16).astype(jnp.float32) for terms in (g_w_gate, g_w_up, g_w_down)]
    gradients = clipped(gradients, sum(jnp.sum(g * g) for g in gradients), sum(g.size for g in gradients))
    new = [
        adamw(w.astype(jnp.float32), m, v, g)
        for w, m, v, g in zip((w_gate, w_up, w_down), (m_w_gate, m_w_up, m_w_down), (v_w_gate, v_w_up, v_w_down), gradients, strict=True)
    ]
    return tuple(one[which] for which in range(3) for one in new)
```

```python
import functools

import jax
import jax.numpy as jnp
from jax import lax
from jax.experimental import pallas as pl
from jax.experimental.pallas import tpu as pltpu
from jax.sharding import PartitionSpec as P

MESH = pl.DeviceIdType.MESH
F32, BF16 = jnp.float32, jnp.bfloat16
ROWS, PAD = 14, 16
BLOCK, TALL = 4 * ROWS, 40
STRIDE = (16, 4, 1)
X, Y, Z = GATE, UP, DOWN = range(3)
PAIR = (0, 1)
ALL = slice(None)
VMEM_LIMIT = 58 * 1024 * 1024


def place():
    me = lax.axis_index("dp")
    c = (lax.div(me, 16), lax.rem(lax.div(me, 4), 4), lax.rem(me, 4))

    def peer(axis, shift):
        return me + (lax.rem(c[axis] + (shift % 4), 4) - c[axis]) * STRIDE[axis]

    return c, peer


def mod4(value):
    return lax.rem(value + 8, 4)


def greet(peers):
    barrier = pltpu.get_barrier_semaphore()
    for p in peers:
        pl.semaphore_signal(barrier, inc=1, device_id={"dp": p}, device_id_type=MESH)
    pl.semaphore_wait(barrier, len(peers))


def tiles(shape, body):
    if len(shape) == 3:
        @pl.loop(0, shape[0])
        def _(i):
            body((i, ALL, ALL))
    elif shape[0] == TALL:
        body((ALL, ALL))
    else:
        width = next(w for w in (512, 256, 128) if shape[1] % w == 0)
        @pl.loop(0, shape[1] // width)
        def _(i):
            body((ALL, pl.ds(pl.multiple_of(i * width, width), width)))


class Copies:
    def __init__(self, send, recv):
        self.send, self.recv, self.next, self.made = send, recv, 0, []

    def remote(self, src, dst, device):
        n = self.next
        self.next += 1
        copy = pltpu.make_async_remote_copy(
            src_ref=src, dst_ref=dst, send_sem=self.send.at[n], recv_sem=self.recv.at[n],
            device_id={"dp": device}, device_id_type=MESH,
        )
        self.made.append(copy)
        return copy

    def drain(self):
        for copy in self.made:
            copy.wait_send()


class Local:
    def __init__(self, sem):
        self.sem, self.next = sem, 0

    def start(self, src, dst):
        copy = pltpu.make_async_copy(src, dst, self.sem.at[self.next])
        self.next += 1
        copy.start()
        return copy


def scatter_kernel(cols, fcols, count, *refs):
    it = iter(refs)
    take = lambda n: [next(it) for _ in range(n)]
    three = lambda: take(3)
    g, w, m, v = three(), three(), three(), three()
    new_w, new_m, new_v = three(), three(), three()
    own1, ro1, rd1, rs1 = three(), three(), three(), three()
    sb2, sf2, ro2, rd2, rs2 = three(), three(), three(), three(), three()
    sb3, sf3, ro3, rd3, rs3 = three(), three(), three(), three(), three()
    fold, four, raw_w, raw_m, raw_v, w32, m32, v32, gf = take(9)
    wd, md, vd, gd = take(4)
    part, parts = take(2)
    send, recv, lsem = three()
    (x, y, z), peer = place()
    c = (x, y, z)
    copies, local = Copies(send, recv), Local(lsem)
    AXES = ((X, Y, Z), (Y, Z, X), (Z, X, Y))
    JAXIS = (Y, X, X)
    SIGN = (1, -1)

    def order(axis, layer):
        s = SIGN[layer]
        return [mod4(c[axis] + d) for d in (2, -s, s, 0)]

    def unit(a, layer, k, j):
        if a == GATE:
            return g[GATE].at[layer, k, j]
        if a == UP:
            return g[UP].at[layer, j, k]
        return g[DOWN].at[layer, j, :, k]

    everyone = [peer(axis, shift) for axis in (X, Y, Z) for shift in (1, 2, 3)]

    small = [local.start(m[a], dst) for a, dst in ((0, raw_m.at[0]), (1, raw_m.at[1]), (2, md))]
    small += [local.start(v[a], dst) for a, dst in ((0, raw_v.at[0]), (1, raw_v.at[1]), (2, vd))]
    small += [local.start(w[a].at[:, x, y], raw_w.at[a]) for a in (0, 1)]
    small += [local.start(w[DOWN].at[:, x, y, z], wd)]

    greet(everyone)

    opp1, dir1, own_s = {}, {}, {}
    for p in range(4):
        for a in range(3):
            for layer in PAIR:
                ax, s, j = AXES[a][0], SIGN[layer], order(JAXIS[a], layer)[p]
                copy = copies.remote(unit(a, layer, mod4(c[ax] + 2), j), ro1[a].at[layer, p], peer(ax, s))
                copy.start()
                opp1[a, layer, p] = copy
                own_s[a, layer, p] = local.start(unit(a, layer, mod4(c[ax] + s), j), own1[a].at[layer, p])
    for p in range(4):
        for a in range(3):
            for layer in PAIR:
                ax, s, j = AXES[a][0], SIGN[layer], order(JAXIS[a], layer)[p]
                copy = copies.remote(unit(a, layer, mod4(c[ax] - s), j), rd1[a].at[layer, p], peer(ax, -s))
                copy.start()
                dir1[a, layer, p] = copy

    fold[BLOCK:64, :] = jnp.zeros((8, cols), F32)

    def part_of(value, at, which):
        fold[(slice(0, BLOCK), at)] = value
        for k in range(4):
            four[(k, ALL, at)] = fold[(slice(k * ROWS, k * ROWS + PAD), at)]
        return [four[(k, ALL, at)] for k in which]

    for copy in small:
        copy.wait()
    for src, dst in ((raw_m, m32), (raw_v, v32)):
        for a in PAIR:
            @pl.loop(0, ROWS)
            def _(r):
                pair = src[a, r]
                dst[a, 0, pl.ds(r, 1), :] = pair[0:1, :]
                dst[a, 1, pl.ds(r, 1), :] = pair[1:2, :]
    for a in PAIR:
        for layer in PAIR:
            def widen(index):
                w32[(a, layer, ALL, index[1])] = part_of(raw_w[(a, layer, *index)].astype(F32), index[1], [z])[0]
            tiles((BLOCK, cols), widen)

    def add(dst, one, two):
        def body(index):
            dst[index] = (one[index].astype(F32) + two[index].astype(F32)).astype(BF16)
        tiles(one.shape, body)

    sum1, own_f = {}, {}
    for p in range(4):
        for a in range(3):
            for layer in PAIR:
                ax, s, j = AXES[a][0], SIGN[layer], order(JAXIS[a], layer)[p]
                opp1[a, layer, p].wait_recv()
                own_s[a, layer, p].wait()
                here = ro1[a].at[layer, p]
                add(here, here, own1[a].at[layer, p])
                copy = copies.remote(here, rs1[a].at[layer, p], peer(ax, s))
                copy.start()
                sum1[a, layer, p] = copy
                own_f[a, layer, p] = local.start(unit(a, layer, c[ax], j), own1[a].at[layer, p])

    def total(one, two, three, index):
        return one[index].astype(F32) + two[index].astype(F32) + three[index].astype(F32)

    def cut(one, two, three, layer, sb, sf):
        pieces = order(Z, layer)

        def body(index):
            at = index[1]
            for role, piece in enumerate(part_of(total(one, two, three, index), at, pieces)):
                if role < 2:
                    sb[(role, ALL, at)] = piece.astype(BF16)
                else:
                    sf[(role - 2, ALL, at)] = piece
        tiles((BLOCK, cols), body)

    opp2, dir2 = {}, {}

    def send2(a, layer, role, src, key):
        ax, s = AXES[a][1], SIGN[layer]
        if role == 0:
            copy = copies.remote(src, ro2[a].at[key], peer(ax, s))
            opp2[(a, *key)] = copy
        else:
            copy = copies.remote(src, rd2[a].at[key], peer(ax, -s))
            dir2[(a, *key)] = copy
        copy.start()

    for p in range(4):
        for a in range(3):
            for layer in PAIR:
                sum1[a, layer, p].wait_recv()
                dir1[a, layer, p].wait_recv()
                own_f[a, layer, p].wait()
                one, two, three = own1[a].at[layer, p], rs1[a].at[layer, p], rd1[a].at[layer, p]
                if a == UP:
                    cut(one, two, three, layer, sb2[UP].at[layer, p], sf2[UP].at[layer, p])
                    send2(1, layer, 0, sb2[UP].at[layer, p, 0], (layer, p))
                    send2(1, layer, 1, sb2[UP].at[layer, p, 1], (layer, p))
                    continue

                def body(index, one=one, two=two, three=three, a=a, layer=layer, p=p):
                    value = total(one, two, three, index)
                    if p < 2:
                        sb2[a][(layer, p, *index)] = value.astype(BF16)
                    else:
                        sf2[a][(layer, p - 2, *index)] = value
                tiles(one.shape, body)
                if p < 2:
                    send2(a, layer, p, sb2[a].at[layer, p], (layer,))

    sum2 = {}

    def pass2(a, layer, key, own):
        opp2[(a, *key)].wait_recv()
        here = ro2[a].at[key]
        add(here, here, own)
        copy = copies.remote(here, rs2[a].at[key], peer(AXES[a][1], SIGN[layer]))
        copy.start()
        sum2[(a, *key)] = copy

    for a in (0, 2):
        for layer in PAIR:
            pass2(a, layer, (layer,), sf2[a].at[layer, 0])
    for p in range(4):
        for layer in PAIR:
            pass2(1, layer, (layer, p), sf2[UP].at[layer, p, 0])

    opp3, dir3, sum3 = {}, {}, {}

    def send3(a, layer, role):
        ax, s = AXES[a][2], SIGN[layer]
        if role == 0:
            opp3[a, layer] = copy = copies.remote(sb3[a].at[layer, 0], ro3[a].at[layer], peer(ax, s))
        else:
            dir3[a, layer] = copy = copies.remote(sb3[a].at[layer, 1], rd3[a].at[layer], peer(ax, -s))
        copy.start()

    for layer in PAIR:
        sum2[0, layer].wait_recv()
        dir2[0, layer].wait_recv()
        cut(sf2[GATE].at[layer, 1], rs2[GATE].at[layer], rd2[GATE].at[layer], layer, sb3[GATE].at[layer], sf3[GATE].at[layer])
        send3(0, layer, 0)
        send3(0, layer, 1)
    for layer in PAIR:
        sum2[2, layer].wait_recv()
        dir2[2, layer].wait_recv()
        for role, k in enumerate(order(Y, layer)):
            value = total(sf2[DOWN].at[layer, 1], rs2[DOWN].at[layer], rd2[DOWN].at[layer], (k, ALL, ALL))
            if role < 2:
                sb3[DOWN][layer, role] = value.astype(BF16)
                send3(2, layer, role)
            else:
                sf3[DOWN][layer, role - 2] = value
    for p in range(4):
        for layer in PAIR:
            sum2[1, layer, p].wait_recv()
            dir2[1, layer, p].wait_recv()

            def body(index, layer=layer, p=p):
                value = total(sf2[UP].at[layer, p, 1], rs2[UP].at[layer, p], rd2[UP].at[layer, p], index)
                if p < 2:
                    sb3[UP][(layer, p, *index)] = value.astype(BF16)
                else:
                    sf3[UP][(layer, p - 2, *index)] = value
            tiles((PAD, cols), body)
            if p < 2:
                send3(1, layer, p)

    for a in (0, 2, 1):
        for layer in PAIR:
            opp3[a, layer].wait_recv()
            here = ro3[a].at[layer]
            add(here, here, sf3[a].at[layer, 0])
            sum3[a, layer] = copy = copies.remote(here, rs3[a].at[layer], peer(AXES[a][2], SIGN[layer]))
            copy.start()

    part[...] = jnp.zeros((8, 128), F32)

    def square(value):
        rows, width = value.shape
        value = value * value
        lines = sum(value[r : r + 8] for r in range(0, rows, 8))
        return sum(lines[:, k : k + 128] for k in range(0, width, 128))

    for a in (0, 2, 1):
        for layer in PAIR:
            sum3[a, layer].wait_recv()
            dir3[a, layer].wait_recv()

            def body(index, a=a, layer=layer):
                value = total(sf3[a].at[layer, 1], rs3[a].at[layer], rd3[a].at[layer], index)
                value = value.astype(BF16).astype(F32)
                if a == DOWN:
                    gd[(layer, *index)] = value
                else:
                    value = jnp.where(lax.broadcasted_iota(jnp.int32, value.shape, 0) < ROWS, value, 0.0)
                    gf[(a, layer, *index)] = value
                part[...] += square(value)
            tiles((TALL, fcols) if a == DOWN else (PAD, cols), body)

    value = part[...]
    for axis in (X, Y, Z):
        mine = parts.at[axis, c[axis]]
        mine[...] = value
        line = [copies.remote(mine, mine, peer(axis, shift)) for shift in (1, 2, 3)]
        for copy in line:
            copy.start()
        for copy in line:
            copy.wait_recv()
        value = (parts[axis, 0] + parts[axis, 1]) + (parts[axis, 2] + parts[axis, 3])
    squares = jnp.full((8, 128), jnp.sum(value), F32)
    factor = jnp.minimum(1.0, 0.5 * lax.rsqrt(squares / count + 1e-30))[0:1, 0:1]

    def adamw(ww, mm, vv, gg):
        gg = gg * factor
        mm = 0.9 * mm + 0.1 * gg
        vv = 0.95 * vv + 0.05 * gg * gg
        step = mm * lax.rsqrt(vv + 1e-8) + 0.1 * ww
        return (ww - 0.02 * step).astype(BF16), mm, vv

    for a in PAIR:
        for layer in PAIR:
            def body(index, a=a, layer=layer):
                at = (a, layer, *index)
                out = (layer, *index)
                new_w[a][out], new_m[a][out], new_v[a][out] = adamw(w32[at], m32[at], v32[at], gf[at])
            tiles((PAD, cols), body)
    for layer in PAIR:
        new_w[DOWN][layer], new_m[DOWN][layer], new_v[DOWN][layer] = adamw(wd[layer].astype(F32), md[layer], vd[layer], gd[layer])
    copies.drain()


def gather_kernel(cols, fcols, *refs):
    it = iter(refs)
    take = lambda n: [next(it) for _ in range(n)]
    three = lambda: take(3)
    own, out = three(), three()
    first, second, fold, send, recv = take(5)
    (x, y, z), peer = place()
    c = (x, y, z)
    copies = Copies(send, recv)
    greet([peer(axis, shift) for axis in (X, Y, Z) for shift in (1, 3)])

    class Ring:
        def __init__(self, axis, slot, source=None):
            self.axis, self.slot = axis, slot
            k = c[axis]
            self.left, self.right = mod4(k - 1), mod4(k + 1)
            self.arrive, self.onward = {}, {}
            for layer in PAIR:
                for side in (1, -1):
                    copy = copies.remote((source or slot)(layer, k), slot(layer, k), peer(axis, side))
                    copy.start()
                    self.arrive[layer, side] = copy

        def forward(self):
            for layer, side, k in ((0, 1, self.left), (1, -1, self.right)):
                self.arrive[layer, side].wait_recv()
                self.onward[layer] = copy = copies.remote(self.slot(layer, k), self.slot(layer, k), peer(self.axis, side))
                copy.start()

        def near(self):
            self.arrive[1, 1].wait_recv()
            self.arrive[0, -1].wait_recv()

        def far(self):
            self.onward[0].wait_recv()
            self.onward[1].wait_recv()

    gate1 = Ring(Z, lambda layer, k: first.at[layer, k], lambda layer, k: own[GATE].at[layer])
    up1 = Ring(X, lambda layer, k: second.at[layer, k, z], lambda layer, k: own[UP].at[layer])
    down1 = Ring(Y, lambda layer, k: out[DOWN].at[layer, x, k, z], lambda layer, k: own[DOWN].at[layer])
    for layer in PAIR:
        first[layer, z] = own[GATE][layer]
        second[layer, x, z] = own[UP][layer]
        out[DOWN][layer, x, y, z] = own[DOWN][layer]

    def up_unit(xb):
        return Ring(Z, lambda layer, k: second.at[layer, xb, k])

    def down_unit(yb):
        return Ring(X, lambda layer, k: out[DOWN].at[layer, k, yb, z])

    def compact(pieces, dst):
        def body(index):
            at = index[1]
            for k in range(4):
                fold[(pl.ds(k * ROWS, PAD), at)] = pieces[(k, ALL, at)].astype(F32)
            dst[(ALL, at)] = fold[(slice(0, BLOCK), at)].astype(BF16)
        tiles((BLOCK, cols), body)

    gate1.forward()
    up1.forward()
    down1.forward()
    up2, down2 = [up_unit(x)], [down_unit(y)]
    gate1.near()
    gate1.far()
    for layer in PAIR:
        compact(first.at[layer], out[GATE].at[layer, x, y])
    gate2 = Ring(Y, lambda layer, k: out[GATE].at[layer, x, k])

    def gate_unit(yb):
        return Ring(X, lambda layer, k: out[GATE].at[layer, k, yb])

    def up_last(xb):
        for layer in PAIR:
            compact(second.at[layer, xb], out[UP].at[layer, xb, y])
        return Ring(Y, lambda layer, k: out[UP].at[layer, xb, k])

    def down_last(xb):
        return Ring(Z, lambda layer, k: out[DOWN].at[layer, xb, :, k])

    up1.near()
    down1.near()
    up2 += [up_unit(mod4(x - 1)), up_unit(mod4(x + 1))]
    down2 += [down_unit(mod4(y - 1)), down_unit(mod4(y + 1))]
    up1.far()
    down1.far()
    up2 += [up_unit(mod4(x + 2))]
    down2 += [down_unit(mod4(y + 2))]
    gate3 = [gate_unit(y)]
    down3 = [down_last(x)]
    for ring in up2 + down2:
        ring.forward()
    gate2.forward()
    up2[0].near()
    up2[0].far()
    up3 = [up_last(x)]
    gate2.near()
    gate3 += [gate_unit(mod4(y - 1)), gate_unit(mod4(y + 1))]
    for ring in down2:
        ring.near()
    down3 += [down_last(mod4(x - 1)), down_last(mod4(x + 1))]
    for ring, xb in zip(up2[1:], (mod4(x - 1), mod4(x + 1), mod4(x + 2))):
        ring.near()
        ring.far()
        up3.append(up_last(xb))
    gate2.far()
    gate3.append(gate_unit(mod4(y + 2)))
    for ring in down2:
        ring.far()
    down3.append(down_last(mod4(x + 2)))
    for rings in zip(gate3, up3, down3):
        for ring in rings:
            ring.forward()
    for rings in zip(gate3, up3, down3):
        for ring in rings:
            ring.near()
            ring.far()
    copies.drain()


def write_kernel(*refs):
    it = iter(refs)
    take = lambda n: [next(it) for _ in range(n)]
    three = lambda: take(3)
    w, m, v = three(), three(), three()
    out_w, out_m, out_v = three(), three(), three()
    pairs, sem = take(2)
    local = Local(sem)
    copies = [local.start(w[a].at[layer, xb], out_w[a].at[layer, xb]) for a in range(3) for layer in (0, 1) for xb in range(4)]
    copies += [local.start(m[DOWN], out_m[DOWN]), local.start(v[DOWN], out_v[DOWN])]
    for n, (src, dst) in enumerate(((m[GATE], out_m[GATE]), (m[UP], out_m[UP]), (v[GATE], out_v[GATE]), (v[UP], out_v[UP]))):
        @pl.loop(0, ROWS)
        def _(r):
            for layer in PAIR:
                pairs[n, r, layer : layer + 1, :] = src[layer, pl.ds(r, 1), :]
        copies.append(local.start(pairs.at[n], dst))
    for copy in copies:
        copy.wait()


def solution(mesh):
    def step(*arrays):
        terms, weights, m, v = (arrays[i : i + 3] for i in (0, 3, 6, 9))
        cols, fcols = terms[0].shape[-1], terms[2].shape[-1]
        rows, frows = terms[0].shape[-2], terms[2].shape[-2]
        assert rows == 64 * ROWS and frows == 64 * TALL
        wide = lambda t: t.reshape(2, 4, 4, 4 * ROWS, cols)
        tall = lambda t: t.reshape(2, 4, 4, 4, TALL, fcols)
        shaped = lambda three: (wide(three[0]), wide(three[1]), tall(three[2]))
        turned = lambda three: (three[0].transpose(1, 0, 2), three[1].transpose(1, 0, 2), three[2])
        count = 2 * (2 * rows * cols + frows * fcols)
        anywhere, on_chip = pl.BlockSpec(memory_space=pl.ANY), pl.BlockSpec(memory_space=pltpu.VMEM)
        B, F = (lambda *shape: pltpu.VMEM(shape, BF16)), (lambda *shape: pltpu.VMEM(shape, F32))
        unit1 = ((BLOCK, cols), (BLOCK, cols), (4, TALL, fcols))
        unit2 = ((2, BLOCK, cols), (2, 4, PAD, cols), (2, 4, TALL, fcols))
        two2 = ((2, 2, BLOCK, cols), (2, 4, 2, PAD, cols), (2, 2, 4, TALL, fcols))
        unit3 = ((PAD, cols), (PAD, cols), (TALL, fcols))
        scratch = [B(2, 4, *u) for _ in range(4) for u in unit1]
        scratch += [B(*u) for u in two2] + [F(*u) for u in two2]
        scratch += [B(*u) for _ in range(3) for u in unit2]
        scratch += [B(2, 2, *u) for u in unit3] + [F(2, 2, *u) for u in unit3]
        scratch += [B(2, *u) for _ in range(3) for u in unit3]
        scratch += [F(64, cols), F(4, PAD, cols), B(2, 2, BLOCK, cols), F(2, ROWS, 2, cols), F(2, ROWS, 2, cols)]
        scratch += [F(2, 2, PAD, cols)] * 4
        scratch += [B(2, TALL, fcols), F(2, TALL, fcols), F(2, TALL, fcols), F(2, TALL, fcols)]
        scratch += [F(8, 128), F(3, 4, 8, 128)]
        scratch += [pltpu.SemaphoreType.DMA((135,)), pltpu.SemaphoreType.DMA((135,)), pltpu.SemaphoreType.DMA((57,))]
        small = [(2, PAD, cols), (2, PAD, cols), (2, TALL, fcols)]
        made = pl.pallas_call(
            functools.partial(scatter_kernel, cols, fcols, count),
            out_shape=[pltpu.VMEM(s, BF16) for s in small] + [pltpu.VMEM(s, F32) for s in small * 2],
            in_specs=[anywhere] * 12,
            out_specs=[on_chip] * 9,
            scratch_shapes=scratch,
            compiler_params=pltpu.CompilerParams(collective_id=0, has_side_effects=True, vmem_limit_bytes=VMEM_LIMIT),
            name="scatter",
        )(*shaped([t[0] for t in terms]), *shaped(weights), *turned(m), *turned(v))
        big = [(2, 4, 4, BLOCK, cols), (2, 4, 4, BLOCK, cols), (2, 4, 4, 4, TALL, fcols)]
        whole = pl.pallas_call(
            functools.partial(gather_kernel, cols, fcols),
            out_shape=[pltpu.VMEM(s, BF16) for s in big],
            in_specs=[on_chip] * 3,
            out_specs=[on_chip] * 3,
            scratch_shapes=[B(2, 4, PAD, cols), B(2, 4, 4, PAD, cols), F(64, cols), pltpu.SemaphoreType.DMA((144,)), pltpu.SemaphoreType.DMA((144,))],
            compiler_params=pltpu.CompilerParams(collective_id=1, has_side_effects=True, vmem_limit_bytes=16 * 1024 * 1024),
            name="gather",
        )(*made[:3])
        turned_small = [(ROWS, 2, cols), (ROWS, 2, cols), (2, TALL, fcols)]
        outs = pl.pallas_call(
            write_kernel,
            out_shape=[jax.ShapeDtypeStruct(s, BF16) for s in big] + [jax.ShapeDtypeStruct(s, F32) for s in turned_small * 2],
            in_specs=[on_chip] * 9,
            out_specs=[anywhere] * 9,
            scratch_shapes=[F(4, ROWS, 2, cols), pltpu.SemaphoreType.DMA((30,))],
            compiler_params=pltpu.CompilerParams(vmem_limit_bytes=16 * 1024 * 1024),
            name="write",
        )(*whole, *made[3:])
        back = lambda three: tuple(t.transpose(1, 0, 2) for t in three[:2]) + (three[2],)
        news = tuple(one.reshape(w.shape) for one, w in zip(outs[:3], weights, strict=True))
        return (*news, *back(outs[3:6]), *back(outs[6:9]))

    all_of, cut = P(None, None, None), P(None, "dp", None)
    return jax.shard_map(
        step,
        mesh=mesh,
        in_specs=(P(("rep", "dp"), None, None, None),) * 3 + (all_of,) * 3 + (cut,) * 6,
        out_specs=(P("rep", None, None),) * 3 + (P("rep", "dp", None),) * 6,
        check_vma=False,
    )
```

```python
import functools

import jax
import jax.numpy as jnp
from jax import lax
from jax.experimental import pallas as pl
from jax.experimental.pallas import tpu as pltpu
from jax.sharding import PartitionSpec as P

MESH = pl.DeviceIdType.MESH
F32, BF16 = jnp.float32, jnp.bfloat16
ROWS, PAD = 14, 16
BLOCK, TALL = 4 * ROWS, 40
STRIDE = (16, 4, 1)
X, Y, Z = GATE, UP, DOWN = range(3)
PAIR = (0, 1)
SIGN = (1, -1)
ALL = slice(None)
MIB = 1024 * 1024
STEP_MIB = 34


def place():
    me = lax.axis_index("dp")
    c = (lax.div(me, 16), lax.rem(lax.div(me, 4), 4), lax.rem(me, 4))

    def peer(axis, shift):
        return me + (lax.rem(c[axis] + (shift % 4), 4) - c[axis]) * STRIDE[axis]

    return c, peer


def mod4(value):
    return lax.rem(value + 8, 4)


def greet(peers):
    barrier = pltpu.get_barrier_semaphore()
    for p in peers:
        pl.semaphore_signal(barrier, inc=1, device_id={"dp": p}, device_id_type=MESH)
    pl.semaphore_wait(barrier, len(peers))


class Copies:
    def __init__(self, send, recv):
        self.send, self.recv, self.next, self.made = send, recv, 0, []

    def start(self, src, dst, device):
        n = self.next
        self.next += 1
        copy = pltpu.make_async_remote_copy(
            src_ref=src, dst_ref=dst, send_sem=self.send.at[n], recv_sem=self.recv.at[n],
            device_id={"dp": device}, device_id_type=MESH,
        )
        copy.start()
        self.made.append(copy)
        return copy

    def drain(self):
        for copy in self.made:
            copy.wait_send()
        self.made = []


class Local:
    def __init__(self, sem):
        self.sem, self.next = sem, 0

    def start(self, src, dst):
        copy = pltpu.make_async_copy(src, dst, self.sem.at[self.next])
        self.next += 1
        copy.start()
        return copy


class Ring:
    def __init__(self, copies, c, peer, axis, slot):
        self.copies, self.peer, self.axis, self.slot = copies, peer, axis, slot
        self.k = c[axis]
        self.left, self.right = mod4(self.k - 1), mod4(self.k + 1)
        self.arrive, self.onward = {}, {}

    def start(self, layer):
        here = self.slot(layer, self.k)
        for side in SIGN:
            self.arrive[layer, side] = self.copies.start(here, here, self.peer(self.axis, side))

    def forward(self):
        for layer, k in zip(PAIR, (self.left, self.right)):
            side = SIGN[layer]
            self.arrive[layer, side].wait_recv()
            here = self.slot(layer, k)
            self.onward[layer] = self.copies.start(here, here, self.peer(self.axis, side))

    def near(self):
        for layer in PAIR:
            self.arrive[layer, -SIGN[layer]].wait_recv()

    def far(self):
        for layer in PAIR:
            self.onward[layer].wait_recv()


def step_kernel(cols, count, *refs):
    it = iter(refs)
    take = lambda n: [next(it) for _ in range(n)]
    three = lambda: take(3)
    quarter = cols // 4
    g, w, m, v = three(), three(), three(), three()
    out, new_m, new_v = three(), three(), three()
    sb2, sf2, ro2, rd2, rs2 = three(), three(), three(), three(), three()
    sb3, sf3, ro3, rd3, rs3 = three(), three(), three(), three(), three()
    own_m, own_v, own_w, own_g = three(), three(), three(), three()
    packed = take(2)
    fold, packs, raw_w, raw_m, raw_v, part, parts, send, recv, lsem = take(10)
    (x, y, z), peer = place()
    c = (x, y, z)
    copies, local = Copies(send, recv), Local(lsem)
    AXES = ((X, Y, Z), (Y, Z, X), (Z, X, Y))
    ro1, rd1, rs1, own1 = ([lambda layer, p, a=a, n=n: out[a].at[layer, n, p] for a in range(3)] for n in range(4))
    cases = [(a, layer) for a in range(3) for layer in PAIR]

    def order(axis, layer):
        s = SIGN[layer]
        return [mod4(c[axis] + d) for d in (2, -s, s, 0)]

    def unit(a, layer, k, p):
        if a == GATE:
            return g[a].at[layer, k, order(Y, layer)[p]]
        if a == UP:
            return g[a].at[layer, order(X, layer)[p], k]
        return g[a].at[layer, order(X, layer)[p], :, k]

    small = [local.start(src[a], dst) for src, dsts in ((m, (raw_m.at[GATE], raw_m.at[UP], own_m[DOWN])), (v, (raw_v.at[GATE], raw_v.at[UP], own_v[DOWN]))) for a, dst in enumerate(dsts)]
    small += [local.start(w[a].at[:, x, y], raw_w.at[a]) for a in (GATE, UP)]
    small += [local.start(w[DOWN].at[:, x, y, z], own_w[DOWN])]

    greet([peer(axis, shift) for axis in (X, Y, Z) for shift in (1, 2, 3)])

    opp1, dir1, sum1, mine = {}, {}, {}, {}
    for p in range(4):
        for a, layer in cases:
            ax, s = AXES[a][0], SIGN[layer]
            opp1[a, layer, p] = copies.start(unit(a, layer, mod4(c[ax] + 2), p), ro1[a](layer, p), peer(ax, s))
            mine[a, layer, p] = local.start(unit(a, layer, mod4(c[ax] + s), p), own1[a](layer, p))
    for p in range(4):
        for a, layer in cases:
            ax, s = AXES[a][0], SIGN[layer]
            dir1[a, layer, p] = copies.start(unit(a, layer, mod4(c[ax] - s), p), rd1[a](layer, p), peer(ax, -s))

    def pack(rows):
        for n in range(4):
            fold[0:BLOCK, :] = rows(slice(n * quarter, (n + 1) * quarter))
            for k in range(4):
                packs[k, n * ROWS : n * ROWS + PAD, :] = fold[k * ROWS : k * ROWS + PAD, :]

    def unpack(pieces, dst):
        for k in range(4):
            packs[k, 0:BLOCK, :] = pieces[k].astype(F32)
        for n in range(4):
            for k in range(4):
                fold[k * ROWS : k * ROWS + PAD, :] = packs[k, n * ROWS : n * ROWS + PAD, :]
            dst[:, n * quarter : (n + 1) * quarter] = fold[0:BLOCK, :].astype(BF16)

    fold[BLOCK:, :] = jnp.zeros((64 - BLOCK, quarter), F32)
    packs[:, BLOCK:, :] = jnp.zeros((4, 64 - BLOCK, quarter), F32)
    for copy in small:
        copy.wait()
    for src, dst in ((raw_m, own_m), (raw_v, own_v)):
        for a in (GATE, UP):
            @pl.loop(0, ROWS)
            def _(r):
                rows = src[a, r]
                for layer in PAIR:
                    for n in range(4):
                        dst[a][layer, pl.ds(n * ROWS + r, 1), :] = rows[layer : layer + 1, n * quarter : (n + 1) * quarter]
    for a in (GATE, UP):
        for layer in PAIR:
            pack(lambda at: raw_w[a, layer, :, at].astype(F32))
            own_w[a][layer] = packs[z, 0:BLOCK, :]

    def add(dst, one, two):
        if one.shape[0] == 4:
            for k in range(4):
                dst[k] = (one[k].astype(F32) + two[k].astype(F32)).astype(BF16)
        elif one.shape[1] == cols:
            @pl.loop(0, 4)
            def _(n):
                at = pl.ds(pl.multiple_of(n * quarter, quarter), quarter)
                dst[:, at] = (one[:, at].astype(F32) + two[:, at].astype(F32)).astype(BF16)
        else:
            dst[...] = (one[...].astype(F32) + two[...].astype(F32)).astype(BF16)

    def total(refs, at):
        one, two, three = (r[at].astype(F32) for r in refs)
        return one + two + three

    for p in range(4):
        for a, layer in cases:
            ax, s = AXES[a][0], SIGN[layer]
            opp1[a, layer, p].wait_recv()
            mine[a, layer, p].wait()
            here = ro1[a](layer, p)
            add(here, here, own1[a](layer, p))
            sum1[a, layer, p] = copies.start(here, rs1[a](layer, p), peer(ax, s))
            mine[a, layer, p] = local.start(unit(a, layer, c[ax], p), own1[a](layer, p))

    opp2, dir2, sum2 = {}, {}, {}

    def keep2(a, layer, r2, r3, value):
        ax, s = AXES[a][1], SIGN[layer]
        if r2 >= 2:
            sf2[a][layer, r2 - 2, r3] = value
            return
        sb2[a][layer, r2, r3] = value.astype(BF16)
        here = sb2[a].at[layer, r2, r3]
        if r2 == 0:
            opp2[a, layer, r3] = copies.start(here, ro2[a].at[layer, r3], peer(ax, s))
        else:
            dir2[a, layer, r3] = copies.start(here, rd2[a].at[layer, r3], peer(ax, -s))

    for p in range(4):
        for a, layer in cases:
            sum1[a, layer, p].wait_recv()
            dir1[a, layer, p].wait_recv()
            mine[a, layer, p].wait()
            terms = [b[a](layer, p) for b in (own1, rs1, rd1)]
            pieces = order(Y if a == DOWN else Z, layer)
            if a == DOWN:
                for q, k in enumerate(pieces):
                    keep2(a, layer, p, q, total(terms, k))
                continue
            pack(lambda at: total(terms, (ALL, at)))
            for q, k in enumerate(pieces):
                r2, r3 = (q, p) if a == UP else (p, q)
                keep2(a, layer, r2, r3, packs[k, 0:BLOCK, :])

    for r3 in range(4):
        for a, layer in cases:
            opp2[a, layer, r3].wait_recv()
            here = ro2[a].at[layer, r3]
            add(here, here, sf2[a].at[layer, 0, r3])
            sum2[a, layer, r3] = copies.start(here, rs2[a].at[layer, r3], peer(AXES[a][1], SIGN[layer]))
    copies.drain()

    opp3, dir3, sum3 = {}, {}, {}
    for r3 in range(4):
        for a, layer in cases:
            ax, s = AXES[a][2], SIGN[layer]
            sum2[a, layer, r3].wait_recv()
            dir2[a, layer, r3].wait_recv()
            value = total((sf2[a].at[layer, 1, r3], rs2[a].at[layer, r3], rd2[a].at[layer, r3]), ...)
            if r3 >= 2:
                sf3[a][layer, r3 - 2] = value
                continue
            sb3[a][layer, r3] = value.astype(BF16)
            here = sb3[a].at[layer, r3]
            if r3 == 0:
                opp3[a, layer] = copies.start(here, ro3[a].at[layer], peer(ax, s))
            else:
                dir3[a, layer] = copies.start(here, rd3[a].at[layer], peer(ax, -s))
        if r3 == 2:
            for a, layer in cases:
                opp3[a, layer].wait_recv()
                here = ro3[a].at[layer]
                add(here, here, sf3[a].at[layer, 0])
                sum3[a, layer] = copies.start(here, rs3[a].at[layer], peer(AXES[a][2], SIGN[layer]))

    part[...] = jnp.zeros((8, 128), F32)
    for a, layer in cases:
        sum3[a, layer].wait_recv()
        dir3[a, layer].wait_recv()
        value = total((sf3[a].at[layer, 1], rs3[a].at[layer], rd3[a].at[layer]), ...)
        value = value.astype(BF16).astype(F32)
        own_g[a][layer] = value
        value = value * value
        lines = sum(value[r : r + 8] for r in range(0, value.shape[0], 8))
        part[...] += sum(lines[:, k : k + 128] for k in range(0, value.shape[1], 128))

    value = part[...]
    for axis in (X, Y, Z):
        own = parts.at[axis, c[axis]]
        own[...] = value
        line = [copies.start(own, own, peer(axis, shift)) for shift in (1, 2, 3)]
        for copy in line:
            copy.wait_recv()
        value = (parts[axis, 0] + parts[axis, 1]) + (parts[axis, 2] + parts[axis, 3])
    squares = jnp.full((8, 128), jnp.sum(value), F32)
    factor = jnp.minimum(1.0, 0.5 * lax.rsqrt(squares / count + 1e-30))[0:1, 0:1]

    ring = functools.partial(Ring, copies, c, peer)

    def piece(a, i, j):
        if a == DOWN:
            return lambda layer: out[a].at[layer, i, j, z]
        return lambda layer: packed[a].at[layer, i, j]

    def slot1(a):
        if a == UP:
            return lambda layer, k: piece(a, k, z)(layer)
        return lambda layer, k: piece(a, y if a == GATE else x, k)(layer)

    def slot2(a, fixed):
        if a == UP:
            return lambda layer, k: piece(a, fixed, k)(layer)
        return lambda layer, k: piece(a, k, fixed)(layer)

    def slot3(a, fixed):
        if a == GATE:
            return lambda layer, k: out[a].at[layer, k, fixed]
        if a == UP:
            return lambda layer, k: out[a].at[layer, fixed, k]
        return lambda layer, k: out[a].at[layer, fixed, :, k]

    def near_first(axis):
        return [mod4(c[axis] + d) for d in (0, -1, 1, 2)]

    first = [ring(AXES[a][2], slot1(a)) for a in range(3)]
    second = [[ring(AXES[a][1], slot2(a, k)) for k in near_first(AXES[a][2])] for a in range(3)]
    BLOCKS = (Y, X, X)
    third = [[ring(AXES[a][0], slot3(a, k)) for k in near_first(BLOCKS[a])] for a in range(3)]

    for a, layer in cases:
        gg = own_g[a][layer] * factor
        ww = own_w[a][layer].astype(F32)
        mm = 0.9 * own_m[a][layer] + 0.1 * gg
        vv = 0.95 * own_v[a][layer] + 0.05 * gg * gg
        new_m[a][layer], new_v[a][layer] = mm, vv
        here = first[a].slot(layer, c[AXES[a][2]])
        here[...] = (ww - 0.02 * (mm * lax.rsqrt(vv + 1e-8) + 0.1 * ww)).astype(BF16)
        first[a].start(layer)
        second[a][0].start(layer)

    def last(a, n):
        k = near_first(BLOCKS[a])[n]
        for layer in PAIR:
            if a != DOWN:
                unpack(packed[a].at[layer, k], third[a][n].slot(layer, c[AXES[a][0]]))
            third[a][n].start(layer)

    for r in first:
        r.forward()
    for a in range(3):
        first[a].near()
        for r in second[a][1:3]:
            for layer in PAIR:
                r.start(layer)
    for a in range(3):
        first[a].far()
        for layer in PAIR:
            second[a][3].start(layer)
    last(DOWN, 0)
    last(GATE, 0)
    for n in range(4):
        for a in range(3):
            second[a][n].forward()
        if n == 1:
            second[UP][0].near()
            second[UP][0].far()
            last(UP, 0)
    for a in (DOWN, GATE):
        for r in second[a]:
            r.near()
        last(a, 1)
        last(a, 2)
    for n in range(1, 4):
        second[UP][n].near()
        second[UP][n].far()
        last(UP, n)
    for a in (DOWN, GATE):
        for r in second[a]:
            r.far()
        last(a, 3)
    for n in range(4):
        for a in range(3):
            third[a][n].forward()
    for n in range(4):
        for a in range(3):
            third[a][n].near()
            third[a][n].far()
    copies.drain()


def write_kernel(*refs):
    it = iter(refs)
    take = lambda n: [next(it) for _ in range(n)]
    three = lambda: take(3)
    w, m, v = three(), three(), three()
    out_w, out_m, out_v = three(), three(), three()
    pairs, sem = take(2)
    quarter = m[GATE].shape[-1]
    local = Local(sem)
    copies = [local.start(w[a].at[layer, k], out_w[a].at[layer, k]) for a in range(3) for layer in PAIR for k in range(4)]
    copies += [local.start(m[DOWN], out_m[DOWN]), local.start(v[DOWN], out_v[DOWN])]
    for i, (src, dst) in enumerate((s[a], d[a]) for s, d in ((m, out_m), (v, out_v)) for a in (GATE, UP)):
        @pl.loop(0, ROWS)
        def _(r):
            for layer in PAIR:
                for n in range(4):
                    pairs[i, r, layer : layer + 1, n * quarter : (n + 1) * quarter] = src[layer, pl.ds(n * ROWS + r, 1), :]
        copies.append(local.start(pairs.at[i], dst))
    for copy in copies:
        copy.wait()


def solution(mesh):
    def step(*arrays):
        terms, weights, m, v = (arrays[i : i + 3] for i in (0, 3, 6, 9))
        cols, fcols = terms[GATE].shape[-1], terms[DOWN].shape[-1]
        rows, frows = terms[GATE].shape[-2], terms[DOWN].shape[-2]
        assert rows == 64 * ROWS and frows == 64 * TALL and cols % 512 == 0
        wide = lambda t: t.reshape(2, 4, 4, BLOCK, cols)
        tall = lambda t: t.reshape(2, 4, 4, 4, TALL, fcols)
        shaped = lambda three: (*map(wide, three[:DOWN]), tall(three[DOWN]))
        turn = lambda t: t.transpose(1, 0, 2)
        turned = lambda three: (*map(turn, three[:DOWN]), three[DOWN])
        count = 2 * (2 * rows * cols + frows * fcols)
        anywhere, on_chip = pl.BlockSpec(memory_space=pl.ANY), pl.BlockSpec(memory_space=pltpu.VMEM)
        piece = (BLOCK, cols // 4)
        pieces = (piece, piece, (TALL, fcols))
        every = lambda dtype, *lead: [pltpu.VMEM((*lead, *p), dtype) for p in pieces]
        scratch = [*every(BF16, 2, 2, 4), *every(F32, 2, 2, 4), *every(BF16, 2, 4), *every(BF16, 2, 4), *every(BF16, 2, 4)]
        scratch += [*every(BF16, 2, 2), *every(F32, 2, 2), *every(BF16, 2), *every(BF16, 2), *every(BF16, 2)]
        scratch += [*every(F32, 2), *every(F32, 2), *every(F32, 2)[:DOWN], every(BF16, 2)[DOWN], *every(F32, 2)]
        scratch += every(BF16, 2, 4, 4)[:DOWN]
        scratch += [pltpu.VMEM((64, cols // 4), F32), pltpu.VMEM((4, 64, cols // 4), F32), pltpu.VMEM((2, 2, BLOCK, cols), BF16)]
        scratch += [pltpu.VMEM((2, ROWS, 2, cols), F32)] * 2
        scratch += [pltpu.VMEM((8, 128), F32), pltpu.VMEM((3, 4, 8, 128), F32)]
        scratch += [pltpu.SemaphoreType.DMA((n,)) for n in (333, 333, 57)]
        big = [(2, 4, 4, BLOCK, cols), (2, 4, 4, BLOCK, cols), (2, 4, 4, 4, TALL, fcols)]
        made = pl.pallas_call(
            functools.partial(step_kernel, cols, count),
            out_shape=[pltpu.VMEM(s, BF16) for s in big] + [pltpu.VMEM((2, *p), F32) for p in pieces * 2],
            in_specs=[anywhere] * 12,
            out_specs=[on_chip] * 9,
            scratch_shapes=scratch,
            compiler_params=pltpu.CompilerParams(collective_id=0, has_side_effects=True, vmem_limit_bytes=STEP_MIB * MIB),
            name="step",
        )(*shaped([t[0] for t in terms]), *shaped(weights), *turned(m), *turned(v))
        ends = [(ROWS, 2, cols), (ROWS, 2, cols), (2, TALL, fcols)]
        outs = pl.pallas_call(
            write_kernel,
            out_shape=[jax.ShapeDtypeStruct(s, BF16) for s in big] + [jax.ShapeDtypeStruct(s, F32) for s in ends * 2],
            in_specs=[on_chip] * 9,
            out_specs=[anywhere] * 9,
            scratch_shapes=[pltpu.VMEM((4, ROWS, 2, cols), F32), pltpu.SemaphoreType.DMA((30,))],
            compiler_params=pltpu.CompilerParams(vmem_limit_bytes=16 * MIB),
            name="write",
        )(*made)
        news = tuple(one.reshape(w.shape) for one, w in zip(outs, weights))
        return (*news, *turned(outs[3:6]), *turned(outs[6:9]))

    all_of, cut = P(None, None, None), P(None, "dp", None)
    return jax.shard_map(
        step,
        mesh=mesh,
        in_specs=(P(("rep", "dp"), None, None, None),) * 3 + (all_of,) * 3 + (cut,) * 6,
        out_specs=(P("rep", None, None),) * 3 + (P("rep", "dp", None),) * 6,
        check_vma=False,
    )
```

```python
import functools

import jax
import jax.numpy as jnp
from jax import lax
from jax.experimental import pallas as pl
from jax.experimental.pallas import tpu as pltpu
from jax.sharding import PartitionSpec as P

MESH = pl.DeviceIdType.MESH
F32, BF16 = jnp.float32, jnp.bfloat16
ROWS, PAD = 14, 16
BLOCK, TALL = 4 * ROWS, 40
STRIDE = (16, 4, 1)
X, Y, Z = GATE, UP, DOWN = range(3)
PAIR = (0, 1)
SIGN = (1, -1)
ALL = slice(None)
MIB = 1024 * 1024
STEP_MIB = 34


def place():
    me = lax.axis_index("dp")
    c = (lax.div(me, 16), lax.rem(lax.div(me, 4), 4), lax.rem(me, 4))

    def peer(axis, shift):
        return me + (lax.rem(c[axis] + (shift % 4), 4) - c[axis]) * STRIDE[axis]

    return c, peer


def mod4(value):
    return lax.rem(value + 8, 4)


def greet(peers):
    barrier = pltpu.get_barrier_semaphore()
    for p in peers:
        pl.semaphore_signal(barrier, inc=1, device_id={"dp": p}, device_id_type=MESH)
    pl.semaphore_wait(barrier, len(peers))


class Copies:
    def __init__(self, send, recv):
        self.send, self.recv, self.next, self.made = send, recv, 0, []

    def start(self, src, dst, device):
        n = self.next
        self.next += 1
        copy = pltpu.make_async_remote_copy(
            src_ref=src, dst_ref=dst, send_sem=self.send.at[n], recv_sem=self.recv.at[n],
            device_id={"dp": device}, device_id_type=MESH,
        )
        copy.start()
        self.made.append(copy)
        return copy

    def drain(self):
        for copy in self.made:
            copy.wait_send()
        self.made = []


class Local:
    def __init__(self, sem):
        self.sem, self.next = sem, 0

    def start(self, src, dst):
        copy = pltpu.make_async_copy(src, dst, self.sem.at[self.next])
        self.next += 1
        copy.start()
        return copy


class Ring:
    def __init__(self, copies, c, peer, axis, slot):
        self.copies, self.peer, self.axis, self.slot = copies, peer, axis, slot
        self.k = c[axis]
        self.left, self.right = mod4(self.k - 1), mod4(self.k + 1)
        self.arrive, self.onward = {}, {}

    def start(self, layer):
        here = self.slot(layer, self.k)
        for side in SIGN:
            self.arrive[layer, side] = self.copies.start(here, here, self.peer(self.axis, side))

    def forward(self):
        for layer, k in zip(PAIR, (self.left, self.right)):
            side = SIGN[layer]
            self.arrive[layer, side].wait_recv()
            here = self.slot(layer, k)
            self.onward[layer] = self.copies.start(here, here, self.peer(self.axis, side))

    def near(self):
        for layer in PAIR:
            self.arrive[layer, -SIGN[layer]].wait_recv()

    def far(self):
        for layer in PAIR:
            self.onward[layer].wait_recv()


def step_kernel(cols, count, *refs):
    it = iter(refs)
    take = lambda n: [next(it) for _ in range(n)]
    three = lambda: take(3)
    quarter = cols // 4
    g, w, m, v = three(), three(), three(), three()
    out, new_m, new_v = three(), three(), three()
    sb2, sf2, ro2, rd2, rs2 = three(), three(), three(), three(), three()
    sb3, sf3, ro3, rd3, rs3 = three(), three(), three(), three(), three()
    own_m, own_v, own_w, own_g = three(), three(), three(), three()
    packed = take(2)
    fold, packs, raw_w, raw_m, raw_v, part, parts, send, recv, lsem = take(10)
    (x, y, z), peer = place()
    c = (x, y, z)
    copies, local = Copies(send, recv), Local(lsem)
    AXES = ((X, Y, Z), (Y, Z, X), (Z, X, Y))
    ro1, rd1, rs1, own1 = ([lambda layer, p, a=a, n=n: out[a].at[layer, n, p] for a in range(3)] for n in range(4))
    cases = [(a, layer) for a in range(3) for layer in PAIR]

    def order(axis, layer):
        s = SIGN[layer]
        return [mod4(c[axis] + d) for d in (2, -s, s, 0)]

    def unit(a, layer, k, p):
        if a == GATE:
            return g[a].at[layer, k, order(Y, layer)[p]]
        if a == UP:
            return g[a].at[layer, order(X, layer)[p], k]
        return g[a].at[layer, order(X, layer)[p], :, k]

    small = [local.start(src[a], dst) for src, dsts in ((m, (raw_m.at[GATE], raw_m.at[UP], own_m[DOWN])), (v, (raw_v.at[GATE], raw_v.at[UP], own_v[DOWN]))) for a, dst in enumerate(dsts)]
    small += [local.start(w[a].at[:, x, y], raw_w.at[a]) for a in (GATE, UP)]
    small += [local.start(w[DOWN].at[:, x, y, z], own_w[DOWN])]

    greet([peer(axis, shift) for axis in (X, Y, Z) for shift in (1, 2, 3)])

    opp1, dir1, sum1, mine = {}, {}, {}, {}
    for p in range(4):
        for a, layer in cases:
            ax, s = AXES[a][0], SIGN[layer]
            opp1[a, layer, p] = copies.start(unit(a, layer, mod4(c[ax] + 2), p), ro1[a](layer, p), peer(ax, s))
            mine[a, layer, p] = local.start(unit(a, layer, mod4(c[ax] + s), p), own1[a](layer, p))
    for p in range(4):
        for a, layer in cases:
            ax, s = AXES[a][0], SIGN[layer]
            dir1[a, layer, p] = copies.start(unit(a, layer, mod4(c[ax] - s), p), rd1[a](layer, p), peer(ax, -s))

    def pack(rows):
        for n in range(4):
            fold[0:BLOCK, :] = rows(slice(n * quarter, (n + 1) * quarter))
            for k in range(4):
                packs[k, n * ROWS : n * ROWS + PAD, :] = fold[k * ROWS : k * ROWS + PAD, :]

    def unpack(pieces, dst):
        for k in range(4):
            packs[k, 0:BLOCK, :] = pieces[k].astype(F32)
        for n in range(4):
            for k in range(4):
                fold[k * ROWS : k * ROWS + PAD, :] = packs[k, n * ROWS : n * ROWS + PAD, :]
            dst[:, n * quarter : (n + 1) * quarter] = fold[0:BLOCK, :].astype(BF16)

    fold[BLOCK:, :] = jnp.zeros((64 - BLOCK, quarter), F32)
    packs[:, BLOCK:, :] = jnp.zeros((4, 64 - BLOCK, quarter), F32)
    for copy in small:
        copy.wait()
    for src, dst in ((raw_m, own_m), (raw_v, own_v)):
        for a in (GATE, UP):
            @pl.loop(0, ROWS)
            def _(r):
                rows = src[a, r]
                for layer in PAIR:
                    for n in range(4):
                        dst[a][layer, pl.ds(n * ROWS + r, 1), :] = rows[layer : layer + 1, n * quarter : (n + 1) * quarter]
    for a in (GATE, UP):
        for layer in PAIR:
            pack(lambda at: raw_w[a, layer, :, at].astype(F32))
            own_w[a][layer] = packs[z, 0:BLOCK, :]

    def add(dst, one, two):
        if one.shape[0] == 4:
            for k in range(4):
                dst[k] = (one[k].astype(F32) + two[k].astype(F32)).astype(BF16)
        elif one.shape[1] == cols:
            @pl.loop(0, 4)
            def _(n):
                at = pl.ds(pl.multiple_of(n * quarter, quarter), quarter)
                dst[:, at] = (one[:, at].astype(F32) + two[:, at].astype(F32)).astype(BF16)
        else:
            dst[...] = (one[...].astype(F32) + two[...].astype(F32)).astype(BF16)

    def total(refs, at):
        one, two, three = (r[at].astype(F32) for r in refs)
        return one + two + three

    for p in range(4):
        for a, layer in cases:
            ax, s = AXES[a][0], SIGN[layer]
            opp1[a, layer, p].wait_recv()
            mine[a, layer, p].wait()
            here = ro1[a](layer, p)
            add(here, here, own1[a](layer, p))
            sum1[a, layer, p] = copies.start(here, rs1[a](layer, p), peer(ax, s))
            mine[a, layer, p] = local.start(unit(a, layer, c[ax], p), own1[a](layer, p))

    opp2, dir2, sum2 = {}, {}, {}

    def keep2(a, layer, r2, r3, value):
        ax, s = AXES[a][1], SIGN[layer]
        if r2 >= 2:
            sf2[a][layer, r2 - 2, r3] = value
            return
        sb2[a][layer, r2, r3] = value.astype(BF16)
        here = sb2[a].at[layer, r2, r3]
        if r2 == 0:
            opp2[a, layer, r3] = copies.start(here, ro2[a].at[layer, r3], peer(ax, s))
        else:
            dir2[a, layer, r3] = copies.start(here, rd2[a].at[layer, r3], peer(ax, -s))

    for p in range(4):
        for a, layer in cases:
            sum1[a, layer, p].wait_recv()
            dir1[a, layer, p].wait_recv()
            mine[a, layer, p].wait()
            terms = [b[a](layer, p) for b in (own1, rs1, rd1)]
            pieces = order(Y if a == DOWN else Z, layer)
            if a == DOWN:
                for q, k in enumerate(pieces):
                    keep2(a, layer, p, q, total(terms, k))
                continue
            pack(lambda at: total(terms, (ALL, at)))
            for q, k in enumerate(pieces):
                r2, r3 = (q, p) if a == UP else (p, q)
                keep2(a, layer, r2, r3, packs[k, 0:BLOCK, :])

    for r3 in range(4):
        for a, layer in cases:
            opp2[a, layer, r3].wait_recv()
            here = ro2[a].at[layer, r3]
            add(here, here, sf2[a].at[layer, 0, r3])
            sum2[a, layer, r3] = copies.start(here, rs2[a].at[layer, r3], peer(AXES[a][1], SIGN[layer]))
    copies.drain()

    opp3, dir3, sum3 = {}, {}, {}
    for r3 in range(4):
        for a, layer in cases:
            ax, s = AXES[a][2], SIGN[layer]
            sum2[a, layer, r3].wait_recv()
            dir2[a, layer, r3].wait_recv()
            value = total((sf2[a].at[layer, 1, r3], rs2[a].at[layer, r3], rd2[a].at[layer, r3]), ...)
            if r3 >= 2:
                sf3[a][layer, r3 - 2] = value
                continue
            sb3[a][layer, r3] = value.astype(BF16)
            here = sb3[a].at[layer, r3]
            if r3 == 0:
                opp3[a, layer] = copies.start(here, ro3[a].at[layer], peer(ax, s))
            else:
                dir3[a, layer] = copies.start(here, rd3[a].at[layer], peer(ax, -s))
        if r3 == 2:
            for a, layer in cases:
                opp3[a, layer].wait_recv()
                here = ro3[a].at[layer]
                add(here, here, sf3[a].at[layer, 0])
                sum3[a, layer] = copies.start(here, rs3[a].at[layer], peer(AXES[a][2], SIGN[layer]))

    part[...] = jnp.zeros((8, 128), F32)
    for a, layer in cases:
        sum3[a, layer].wait_recv()
        dir3[a, layer].wait_recv()
        value = total((sf3[a].at[layer, 1], rs3[a].at[layer], rd3[a].at[layer]), ...)
        value = value.astype(BF16).astype(F32)
        own_g[a][layer] = value
        value = value * value
        lines = sum(value[r : r + 8] for r in range(0, value.shape[0], 8))
        part[...] += sum(lines[:, k : k + 128] for k in range(0, value.shape[1], 128))

    value = part[...]
    for axis in (X, Y, Z):
        own = parts.at[axis, c[axis]]
        own[...] = value
        line = [copies.start(own, own, peer(axis, shift)) for shift in (1, 2, 3)]
        for copy in line:
            copy.wait_recv()
        value = (parts[axis, 0] + parts[axis, 1]) + (parts[axis, 2] + parts[axis, 3])
    squares = jnp.full((8, 128), jnp.sum(value), F32)
    factor = jnp.minimum(1.0, 0.5 * lax.rsqrt(squares / count + 1e-30))[0:1, 0:1]

    ring = functools.partial(Ring, copies, c, peer)

    def piece(a, i, j):
        if a == DOWN:
            return lambda layer: out[a].at[layer, i, j, z]
        return lambda layer: packed[a].at[layer, i, j]

    def slot1(a):
        if a == UP:
            return lambda layer, k: piece(a, k, z)(layer)
        return lambda layer, k: piece(a, y if a == GATE else x, k)(layer)

    def slot2(a, fixed):
        if a == UP:
            return lambda layer, k: piece(a, fixed, k)(layer)
        return lambda layer, k: piece(a, k, fixed)(layer)

    def slot3(a, fixed):
        if a == GATE:
            return lambda layer, k: out[a].at[layer, k, fixed]
        if a == UP:
            return lambda layer, k: out[a].at[layer, fixed, k]
        return lambda layer, k: out[a].at[layer, fixed, :, k]

    def near_first(axis):
        return [mod4(c[axis] + d) for d in (0, -1, 1, 2)]

    first = [ring(AXES[a][2], slot1(a)) for a in range(3)]
    second = [[ring(AXES[a][1], slot2(a, k)) for k in near_first(AXES[a][2])] for a in range(3)]
    BLOCKS = (Y, X, X)
    third = [[ring(AXES[a][0], slot3(a, k)) for k in near_first(BLOCKS[a])] for a in range(3)]

    for a, layer in cases:
        gg = own_g[a][layer] * factor
        ww = own_w[a][layer].astype(F32)
        mm = 0.9 * own_m[a][layer] + 0.1 * gg
        vv = 0.95 * own_v[a][layer] + 0.05 * gg * gg
        new_m[a][layer], new_v[a][layer] = mm, vv
        here = first[a].slot(layer, c[AXES[a][2]])
        here[...] = (ww - 0.02 * (mm * lax.rsqrt(vv + 1e-8) + 0.1 * ww)).astype(BF16)
        first[a].start(layer)
        second[a][0].start(layer)

    def last(a, n):
        k = near_first(BLOCKS[a])[n]
        for layer in PAIR:
            if a != DOWN:
                unpack(packed[a].at[layer, k], third[a][n].slot(layer, c[AXES[a][0]]))
            third[a][n].start(layer)

    for r in first:
        r.forward()
    for a in range(3):
        first[a].near()
        for r in second[a][1:3]:
            for layer in PAIR:
                r.start(layer)
    for a in range(3):
        first[a].far()
        for layer in PAIR:
            second[a][3].start(layer)
    last(DOWN, 0)
    last(GATE, 0)
    for n in range(4):
        for a in range(3):
            second[a][n].forward()
        if n == 1:
            second[UP][0].near()
            second[UP][0].far()
            last(UP, 0)
    for a in (DOWN, GATE):
        for r in second[a]:
            r.near()
        last(a, 1)
        last(a, 2)
    for n in range(1, 4):
        second[UP][n].near()
        second[UP][n].far()
        last(UP, n)
    for a in (DOWN, GATE):
        for r in second[a]:
            r.far()
        last(a, 3)
    for n in range(4):
        for a in range(3):
            third[a][n].forward()
    for n in range(4):
        for a in range(3):
            third[a][n].near()
            third[a][n].far()
    copies.drain()


def write_kernel(*refs):
    it = iter(refs)
    take = lambda n: [next(it) for _ in range(n)]
    three = lambda: take(3)
    w, m, v = three(), three(), three()
    out_w, out_m, out_v = three(), three(), three()
    pairs, sem = take(2)
    quarter = m[GATE].shape[-1]
    local = Local(sem)
    copies = [local.start(w[a].at[layer, k], out_w[a].at[layer, k]) for a in range(3) for layer in PAIR for k in range(4)]
    copies += [local.start(m[DOWN], out_m[DOWN]), local.start(v[DOWN], out_v[DOWN])]
    for i, (src, dst) in enumerate((s[a], d[a]) for s, d in ((m, out_m), (v, out_v)) for a in (GATE, UP)):
        @pl.loop(0, ROWS)
        def _(r):
            for layer in PAIR:
                for n in range(4):
                    pairs[i, r, layer : layer + 1, n * quarter : (n + 1) * quarter] = src[layer, pl.ds(n * ROWS + r, 1), :]
        copies.append(local.start(pairs.at[i], dst))
    for copy in copies:
        copy.wait()


def solution(mesh):
    def step(*arrays):
        terms, weights, m, v = (arrays[i : i + 3] for i in (0, 3, 6, 9))
        cols, fcols = terms[GATE].shape[-1], terms[DOWN].shape[-1]
        rows, frows = terms[GATE].shape[-2], terms[DOWN].shape[-2]
        assert rows == 64 * ROWS and frows == 64 * TALL and cols % 512 == 0
        wide = lambda t: t.reshape(2, 4, 4, BLOCK, cols)
        tall = lambda t: t.reshape(2, 4, 4, 4, TALL, fcols)
        shaped = lambda three: (*map(wide, three[:DOWN]), tall(three[DOWN]))
        turn = lambda t: t.transpose(1, 0, 2)
        turned = lambda three: (*map(turn, three[:DOWN]), three[DOWN])
        stay = lambda t: pltpu.with_memory_space_constraint(t, pltpu.HBM)
        count = 2 * (2 * rows * cols + frows * fcols)
        anywhere, on_chip, off_chip = (pl.BlockSpec(memory_space=space) for space in (pl.ANY, pltpu.VMEM, pltpu.HBM))
        piece = (BLOCK, cols // 4)
        pieces = (piece, piece, (TALL, fcols))
        every = lambda dtype, *lead: [pltpu.VMEM((*lead, *p), dtype) for p in pieces]
        scratch = [*every(BF16, 2, 2, 4), *every(F32, 2, 2, 4), *every(BF16, 2, 4), *every(BF16, 2, 4), *every(BF16, 2, 4)]
        scratch += [*every(BF16, 2, 2), *every(F32, 2, 2), *every(BF16, 2), *every(BF16, 2), *every(BF16, 2)]
        scratch += [*every(F32, 2), *every(F32, 2), *every(F32, 2)[:DOWN], every(BF16, 2)[DOWN], *every(F32, 2)]
        scratch += every(BF16, 2, 4, 4)[:DOWN]
        scratch += [pltpu.VMEM((64, cols // 4), F32), pltpu.VMEM((4, 64, cols // 4), F32), pltpu.VMEM((2, 2, BLOCK, cols), BF16)]
        scratch += [pltpu.VMEM((2, ROWS, 2, cols), F32)] * 2
        scratch += [pltpu.VMEM((8, 128), F32), pltpu.VMEM((3, 4, 8, 128), F32)]
        scratch += [pltpu.SemaphoreType.DMA((n,)) for n in (333, 333, 57)]
        big = [(2, 4, 4, BLOCK, cols), (2, 4, 4, BLOCK, cols), (2, 4, 4, 4, TALL, fcols)]
        made = pl.pallas_call(
            functools.partial(step_kernel, cols, count),
            out_shape=[pltpu.VMEM(s, BF16) for s in big] + [pltpu.VMEM((2, *p), F32) for p in pieces * 2],
            in_specs=[off_chip] * 12,
            out_specs=[on_chip] * 9,
            scratch_shapes=scratch,
            compiler_params=pltpu.CompilerParams(collective_id=0, has_side_effects=True, vmem_limit_bytes=STEP_MIB * MIB),
            name="step",
        )(*shaped([t[0] for t in terms]), *shaped(weights), *map(stay, (*turned(m), *turned(v))))
        ends = [(ROWS, 2, cols), (ROWS, 2, cols), (2, TALL, fcols)]
        outs = pl.pallas_call(
            write_kernel,
            out_shape=[jax.ShapeDtypeStruct(s, BF16) for s in big] + [jax.ShapeDtypeStruct(s, F32) for s in ends * 2],
            in_specs=[on_chip] * 9,
            out_specs=[anywhere] * 9,
            scratch_shapes=[pltpu.VMEM((4, ROWS, 2, cols), F32), pltpu.SemaphoreType.DMA((30,))],
            compiler_params=pltpu.CompilerParams(vmem_limit_bytes=2 * MIB),
            name="write",
        )(*made)
        news = tuple(one.reshape(w.shape) for one, w in zip(outs, weights))
        return (*news, *turned(outs[3:6]), *turned(outs[6:9]))

    all_of, cut = P(None, None, None), P(None, "dp", None)
    return jax.shard_map(
        step,
        mesh=mesh,
        in_specs=(P(("rep", "dp"), None, None, None),) * 3 + (all_of,) * 3 + (cut,) * 6,
        out_specs=(P("rep", None, None),) * 3 + (P("rep", "dp", None),) * 6,
        check_vma=False,
    )
```

```python
import functools

import jax
import jax.numpy as jnp
from jax import lax
from jax.experimental import pallas as pl
from jax.experimental.pallas import tpu as pltpu
from jax.sharding import PartitionSpec as P

MESH = pl.DeviceIdType.MESH
F32, BF16 = jnp.float32, jnp.bfloat16
ROWS, PAD = 14, 16
BLOCK, TALL = 4 * ROWS, 40
STRIDE = (16, 4, 1)
X, Y, Z = GATE, UP, DOWN = range(3)
PAIR = (0, 1)
SIGN = (1, -1)
ALL = slice(None)
MIB = 1024 * 1024
STEP_MIB = 34


def place():
    me = lax.axis_index("dp")
    c = (lax.div(me, 16), lax.rem(lax.div(me, 4), 4), lax.rem(me, 4))

    def peer(axis, shift):
        return me + (lax.rem(c[axis] + (shift % 4), 4) - c[axis]) * STRIDE[axis]

    return c, peer


def mod4(value):
    return lax.rem(value + 8, 4)


def greet(peers):
    barrier = pltpu.get_barrier_semaphore()
    for p in peers:
        pl.semaphore_signal(barrier, inc=1, device_id={"dp": p}, device_id_type=MESH)
    pl.semaphore_wait(barrier, len(peers))


class Sends:
    def __init__(self, send, recv):
        self.send, self.recv, self.next = send, recv, 0

    def semaphore(self):
        self.next += 1
        return self.recv.at[self.next - 1]

    def start(self, group, src, dst, device, arrival):
        pltpu.make_async_remote_copy(
            src_ref=src, dst_ref=dst, send_sem=self.send.at[group], recv_sem=arrival, device_id={"dp": device}, device_id_type=MESH
        ).start()


def await_bytes(ref, semaphore):
    pltpu.make_async_copy(ref, ref, semaphore).wait()


class Ring:
    def __init__(self, sends, c, peer, group, axis, slot, onward, near, far):
        self.sends, self.peer, self.group, self.axis, self.slot = sends, peer, group, axis, slot
        self.k = c[axis]
        self.left, self.right = mod4(self.k - 1), mod4(self.k + 1)
        self.onward, self.near, self.far = onward, near, far

    def start(self, layer):
        here = self.slot(layer, self.k)
        self.sends.start(self.group, here, here, self.peer(self.axis, SIGN[layer]), self.onward)
        self.sends.start(self.group, here, here, self.peer(self.axis, -SIGN[layer]), self.near)

    def forward(self):
        await_bytes(self.slot(ALL, self.left), self.onward)
        for layer, k in zip(PAIR, (self.left, self.right)):
            here = self.slot(layer, k)
            self.sends.start(self.group, here, here, self.peer(self.axis, SIGN[layer]), self.far)


def step_kernel(cols, count, *refs):
    it = iter(refs)
    take = lambda n: [next(it) for _ in range(n)]
    three = lambda: take(3)
    quarter = cols // 4
    g, w, m, v = three(), three(), three(), three()
    out, new_m, new_v = three(), three(), three()
    sb2, sf2, ro2, rx2 = three(), three(), three(), three()
    sb3, sf3, ro3, rx3 = three(), three(), three(), three()
    own_m, own_v, own_w, own_g = three(), three(), three(), three()
    packed = take(2)
    fold, packs, raw_w, raw_m, raw_v, parts, send, recv, lsem, psem = take(10)
    (x, y, z), peer = place()
    c = (x, y, z)
    sends = Sends(send, recv)
    AXES = ((X, Y, Z), (Y, Z, X), (Z, X, Y))
    ro1, rd1, rs1, own1 = ([lambda layer, p, a=a, n=n: out[a].at[layer, n, p] for a in range(3)] for n in range(4))
    cases = [(a, p) for p in range(4) for a in range(3)]

    def order(axis, layer):
        s = SIGN[layer]
        return [mod4(c[axis] + d) for d in (2, -s, s, 0)]

    def block(a, layer, k, j):
        if a == GATE:
            return g[a].at[layer, k, j]
        if a == UP:
            return g[a].at[layer, j, k]
        return g[a].at[layer, j, :, k]

    UNITS = (Y, X, X)

    def unit(a, layer, k, p):
        return block(a, layer, k, order(UNITS[a], layer)[p])

    def mine(a, layer, role):
        k = order(AXES[a][0], layer)[role]
        return pltpu.make_async_copy(block(a, layer, k, ALL), out[a].at[layer, 3], lsem.at[2 * a + layer])

    def sent(a, phase):
        if phase == 0:
            ref = out[a].at[:, 0:3]
        elif phase == 1:
            ref = out[a].at[:, 0:3, :, 0] if a == DOWN else packed[a].at[:, 0:3]
        else:
            ref = out[a].at[:, 0:3, 0, 0] if a == DOWN else packed[a].at[:, 0:3, 0]
        await_bytes(ref, send.at[3 * phase + a])

    greet([peer(axis, side) for axis in (X, Y, Z) for side in SIGN])

    opp1, end1 = ({case: sends.semaphore() for case in cases} for _ in range(2))
    for a, p in cases:
        for layer in PAIR:
            ax, s = AXES[a][0], SIGN[layer]
            sends.start(a, unit(a, layer, mod4(c[ax] + 2), p), ro1[a](layer, p), peer(ax, s), opp1[a, p])
            if p == 0:
                mine(a, layer, 2).start()
    for a, p in cases:
        for layer in PAIR:
            ax, s = AXES[a][0], SIGN[layer]
            sends.start(a, unit(a, layer, mod4(c[ax] - s), p), rd1[a](layer, p), peer(ax, -s), end1[a, p])
    small = []
    for n, (src, raw, whole) in enumerate(((m, raw_m, own_m), (v, raw_v, own_v), (w, raw_w, own_w))):
        one, other = lsem.at[6 + n], lsem.at[9 + n]
        for a in (GATE, UP):
            pltpu.make_async_copy(src[a].at[:, x, y] if n == 2 else src[a], raw.at[a], one).start()
        last = pltpu.make_async_copy(src[DOWN].at[:, x, y, z] if n == 2 else src[DOWN], whole[DOWN], other)
        last.start()
        small += [pltpu.make_async_copy(raw, raw, one), last]

    def pack(rows):
        for n in range(4):
            fold[0:BLOCK, :] = rows(slice(n * quarter, (n + 1) * quarter))
            for k in range(4):
                packs[k, n * ROWS : n * ROWS + PAD, :] = fold[k * ROWS : k * ROWS + PAD, :]

    def unpack(pieces, dst):
        for k in range(4):
            packs[k, 0:BLOCK, :] = pieces[k].astype(F32)
        for n in range(4):
            for k in range(4):
                fold[k * ROWS : k * ROWS + PAD, :] = packs[k, n * ROWS : n * ROWS + PAD, :]
            dst[:, n * quarter : (n + 1) * quarter] = fold[0:BLOCK, :].astype(BF16)

    fold[BLOCK:, :] = jnp.zeros((64 - BLOCK, quarter), F32)
    packs[:, BLOCK:, :] = jnp.zeros((4, 64 - BLOCK, quarter), F32)
    for copy in small:
        copy.wait()
    for src, dst in ((raw_m, own_m), (raw_v, own_v)):
        for a in (GATE, UP):
            @pl.loop(0, ROWS)
            def _(r):
                rows = src[a, r]
                for layer in PAIR:
                    for n in range(4):
                        dst[a][layer, pl.ds(n * ROWS + r, 1), :] = rows[layer : layer + 1, n * quarter : (n + 1) * quarter]
    for a in (GATE, UP):
        for layer in PAIR:
            pack(lambda at: raw_w[a, layer, :, at].astype(F32))
            own_w[a][layer] = packs[z, 0:BLOCK, :]

    def add(dst, one, two):
        if one.shape[0] == 4:
            for k in range(4):
                dst[k] = (one[k].astype(F32) + two[k].astype(F32)).astype(BF16)
        elif one.shape[1] == cols:
            @pl.loop(0, 4)
            def _(n):
                at = pl.ds(pl.multiple_of(n * quarter, quarter), quarter)
                dst[:, at] = (one[:, at].astype(F32) + two[:, at].astype(F32)).astype(BF16)
        else:
            dst[...] = (one[...].astype(F32) + two[...].astype(F32)).astype(BF16)

    def total(refs, at):
        one, two, three = (r[at].astype(F32) for r in refs)
        return one + two + three

    for a, p in cases:
        await_bytes(out[a].at[:, 0, p], opp1[a, p])
        for layer in PAIR:
            if p == 0:
                mine(a, layer, 2).wait()
            here = ro1[a](layer, p)
            add(here, here, own1[a](layer, order(UNITS[a], layer)[p]))
            sends.start(a, here, rs1[a](layer, p), peer(AXES[a][0], SIGN[layer]), end1[a, p])
            if p == 3:
                mine(a, layer, 3).start()

    opp2, end2 = ({case: sends.semaphore() for case in cases} for _ in range(2))

    def keep2(a, layer, r2, r3, value):
        ax, s = AXES[a][1], SIGN[layer]
        if r2 >= 2:
            sf2[a][layer, r2 - 2, r3] = value
            return
        sb2[a][layer, r2, r3] = value.astype(BF16)
        here = sb2[a].at[layer, r2, r3]
        if r2 == 0:
            sends.start(3 + a, here, ro2[a].at[layer, r3], peer(ax, s), opp2[a, r3])
        else:
            sends.start(3 + a, here, rx2[a].at[layer, 0, r3], peer(ax, -s), end2[a, r3])

    for a, p in cases:
        await_bytes(out[a].at[:, 1:3, p], end1[a, p])
        for layer in PAIR:
            if p == 0:
                mine(a, layer, 3).wait()
            terms = [own1[a](layer, order(UNITS[a], layer)[p]), rs1[a](layer, p), rd1[a](layer, p)]
            pieces = order(Y if a == DOWN else Z, layer)
            if a == DOWN:
                for q, k in enumerate(pieces):
                    keep2(a, layer, p, q, total(terms, k))
                continue
            pack(lambda at: total(terms, (ALL, at)))
            for q, k in enumerate(pieces):
                r2, r3 = (q, p) if a == UP else (p, q)
                keep2(a, layer, r2, r3, packs[k, 0:BLOCK, :])

    for a, r3 in cases:
        await_bytes(ro2[a].at[:, r3], opp2[a, r3])
        for layer in PAIR:
            here = ro2[a].at[layer, r3]
            add(here, here, sf2[a].at[layer, 0, r3])
            sends.start(3 + a, here, rx2[a].at[layer, 1, r3], peer(AXES[a][1], SIGN[layer]), end2[a, r3])
    for a in range(3):
        sent(a, 0)

    opp3, end3 = ([sends.semaphore() for _ in range(3)] for _ in range(2))
    for a, r3 in cases:
        await_bytes(rx2[a].at[:, :, r3], end2[a, r3])
        for layer in PAIR:
            ax, s = AXES[a][2], SIGN[layer]
            value = total((sf2[a].at[layer, 1, r3], rx2[a].at[layer, 0, r3], rx2[a].at[layer, 1, r3]), ...)
            if r3 >= 2:
                sf3[a][layer, r3 - 2] = value
                continue
            sb3[a][layer, r3] = value.astype(BF16)
            here = sb3[a].at[layer, r3]
            if r3 == 0:
                sends.start(6 + a, here, ro3[a].at[layer], peer(ax, s), opp3[a])
            else:
                sends.start(6 + a, here, rx3[a].at[layer, 0], peer(ax, -s), end3[a])
        if r3 == 2:
            await_bytes(ro3[a], opp3[a])
            for layer in PAIR:
                here = ro3[a].at[layer]
                add(here, here, sf3[a].at[layer, 0])
                sends.start(6 + a, here, rx3[a].at[layer, 1], peer(AXES[a][2], SIGN[layer]), end3[a])

    lines = jnp.zeros((8, 128), F32)
    for a in range(3):
        await_bytes(rx3[a], end3[a])
        for layer in PAIR:
            value = total((sf3[a].at[layer, 1], rx3[a].at[layer, 0], rx3[a].at[layer, 1]), ...)
            value = value.astype(BF16).astype(F32)
            own_g[a][layer] = value
            value = value * value
            value = sum(value[r : r + 8] for r in range(0, value.shape[0], 8))
            lines += sum(value[:, k : k + 128] for k in range(0, value.shape[1], 128))

    me = lax.axis_index("dp")
    parts[me] = jnp.sum(lines, axis=0, keepdims=True)

    @pl.loop(1, 64)
    def _(n):
        pltpu.make_async_remote_copy(
            src_ref=parts.at[me], dst_ref=parts.at[me], send_sem=psem.at[0], recv_sem=psem.at[1],
            device_id={"dp": lax.rem(me + n, 64)}, device_id_type=MESH,
        ).start()
    for a in range(3):
        sent(a, 1)
        sent(a, 2)
    await_bytes(parts.at[0:63], psem.at[1])
    value = jnp.sum(parts[...], axis=0)
    squares = jnp.full((8, 128), jnp.sum(value), F32)
    factor = jnp.minimum(1.0, 0.5 * lax.rsqrt(squares / count + 1e-30))[0:1, 0:1]

    sends.next = 0

    def piece(a, i, j):
        if a == DOWN:
            return lambda layer: out[a].at[layer, i, j, z]
        return lambda layer: packed[a].at[layer, i, j]

    def slot1(a):
        if a == UP:
            return lambda layer, k: piece(a, k, z)(layer)
        return lambda layer, k: piece(a, y if a == GATE else x, k)(layer)

    def slot2(a, fixed):
        if a == UP:
            return lambda layer, k: piece(a, fixed, k)(layer)
        return lambda layer, k: piece(a, k, fixed)(layer)

    def slot3(a, fixed):
        if a == GATE:
            return lambda layer, k: out[a].at[layer, k, fixed]
        if a == UP:
            return lambda layer, k: out[a].at[layer, fixed, k]
        return lambda layer, k: out[a].at[layer, fixed, :, k]

    def near_first(axis):
        return [mod4(c[axis] + d) for d in (0, -1, 1, 2)]

    def rings(a, phase, slot, fixed, shared):
        near, far = (sends.semaphore() for _ in range(2)) if shared else (None, None)
        made = []
        for k in fixed:
            end = None if shared else sends.semaphore()
            made.append(Ring(sends, c, peer, 3 * phase + a, AXES[a][phase], slot(k), sends.semaphore(), near or end, far or end))
        return made

    first = [rings(a, 2, lambda _, a=a: slot1(a), [0], True)[0] for a in range(3)]
    second = [rings(a, 1, functools.partial(slot2, a), near_first(AXES[a][2]), a != UP) for a in range(3)]
    third = [rings(a, 0, functools.partial(slot3, a), near_first(UNITS[a]), False) for a in range(3)]

    for a in range(3):
        for layer in PAIR:
            gg = own_g[a][layer] * factor
            ww = own_w[a][layer].astype(F32)
            mm = 0.9 * own_m[a][layer] + 0.1 * gg
            vv = 0.95 * own_v[a][layer] + 0.05 * gg * gg
            here = first[a].slot(layer, c[AXES[a][2]])
            here[...] = (ww - 0.02 * (mm * lax.rsqrt(vv + 1e-8) + 0.1 * ww)).astype(BF16)
            first[a].start(layer)
            second[a][0].start(layer)
            own_m[a][layer], own_v[a][layer] = mm, vv

    def last(a, n):
        k = near_first(UNITS[a])[n]
        for layer in PAIR:
            if a != DOWN:
                unpack(packed[a].at[layer, k], third[a][n].slot(layer, c[AXES[a][0]]))
            third[a][n].start(layer)

    def near2(a):
        await_bytes(out[a].at[:, 0, :, 0] if a == DOWN else packed[a].at[:, 0], second[a][0].near)

    def far2(a):
        await_bytes(out[a].at[:, 0, :, 0] if a == DOWN else packed[a].at[:, 0], second[a][0].far)

    def up2(n):
        await_bytes(packed[UP].at[:, 0, 0:2], second[UP][n].near)

    for r in first:
        r.forward()
    for a in range(3):
        await_bytes(first[a].slot(ALL, 0), first[a].near)
        for r in second[a][1:3]:
            for layer in PAIR:
                r.start(layer)
    for a in range(3):
        await_bytes(first[a].slot(ALL, 0), first[a].far)
        for layer in PAIR:
            second[a][3].start(layer)
    last(DOWN, 0)
    last(GATE, 0)
    for n in range(4):
        for a in range(3):
            second[a][n].forward()
        if n == 1:
            up2(0)
            last(UP, 0)
    for a in (DOWN, GATE):
        near2(a)
        last(a, 1)
        last(a, 2)
    for n in range(1, 4):
        up2(n)
        last(UP, n)
    for a in (DOWN, GATE):
        far2(a)
        last(a, 3)

    for own, new in ((own_m, new_m), (own_v, new_v)):
        new[DOWN][...] = own[DOWN][...]
        for a in (GATE, UP):
            @pl.loop(0, ROWS)
            def _(r):
                for layer in PAIR:
                    for n in range(4):
                        new[a][r, layer : layer + 1, n * quarter : (n + 1) * quarter] = own[a][layer, pl.ds(n * ROWS + r, 1), :]

    for n in range(4):
        for a in range(3):
            third[a][n].forward()
    for n in range(4):
        for a in range(3):
            await_bytes(out[a].at[:, 0, :, 0:2] if a == DOWN else out[a].at[:, 0, 0:2], third[a][n].far)
    for a in range(3):
        for phase in range(3):
            sent(a, phase)
    await_bytes(parts.at[0:63], psem.at[0])


def write_kernel(*refs):
    *refs, sem = refs
    count = len(refs) // 2
    copies = []
    for n, (src, dst) in reversed(list(enumerate(zip(refs[:count], refs[count:])))):
        copies.append(pltpu.make_async_copy(src, dst, sem.at[n]))
        copies[-1].start()
    for copy in copies:
        copy.wait()


def solution(mesh):
    def step(*arrays):
        terms, weights, m, v = (arrays[i : i + 3] for i in (0, 3, 6, 9))
        cols, fcols = terms[GATE].shape[-1], terms[DOWN].shape[-1]
        rows, frows = terms[GATE].shape[-2], terms[DOWN].shape[-2]
        assert rows == 64 * ROWS and frows == 64 * TALL and cols % 512 == 0
        wide = lambda t: t.reshape(2, 4, 4, BLOCK, cols)
        tall = lambda t: t.reshape(2, 4, 4, 4, TALL, fcols)
        shaped = lambda three: (*map(wide, three[:DOWN]), tall(three[DOWN]))
        turn = lambda t: t.transpose(1, 0, 2)
        turned = lambda three: (*map(turn, three[:DOWN]), three[DOWN])
        stay = lambda t: pltpu.with_memory_space_constraint(t, pltpu.HBM)
        count = 2 * (2 * rows * cols + frows * fcols)
        anywhere, on_chip, off_chip = (pl.BlockSpec(memory_space=space) for space in (pl.ANY, pltpu.VMEM, pltpu.HBM))
        piece = (BLOCK, cols // 4)
        pieces = (piece, piece, (TALL, fcols))
        every = lambda dtype, *lead: [pltpu.VMEM((*lead, *p), dtype) for p in pieces]
        scratch = [*every(BF16, 2, 2, 4), *every(F32, 2, 2, 4), *every(BF16, 2, 4), *every(BF16, 2, 2, 4)]
        scratch += [*every(BF16, 2, 2), *every(F32, 2, 2), *every(BF16, 2), *every(BF16, 2, 2)]
        scratch += [*every(F32, 2), *every(F32, 2), *every(F32, 2)[:DOWN], every(BF16, 2)[DOWN], *every(F32, 2)]
        scratch += every(BF16, 2, 4, 4)[:DOWN]
        scratch += [pltpu.VMEM((64, cols // 4), F32), pltpu.VMEM((4, 64, cols // 4), F32), pltpu.VMEM((2, 2, BLOCK, cols), BF16)]
        scratch += [pltpu.VMEM((2, ROWS, 2, cols), F32)] * 2 + [pltpu.VMEM((64, 1, 128), F32)]
        scratch += [pltpu.SemaphoreType.DMA((n,)) for n in (9, 54, 12, 2)]
        ends = [(ROWS, 2, cols), (ROWS, 2, cols), (2, TALL, fcols)]
        big = [(2, 4, 4, BLOCK, cols), (2, 4, 4, BLOCK, cols), (2, 4, 4, 4, TALL, fcols)]
        made = pl.pallas_call(
            functools.partial(step_kernel, cols, count),
            out_shape=[pltpu.VMEM(s, BF16) for s in big] + [pltpu.VMEM(s, F32) for s in ends * 2],
            in_specs=[off_chip] * 12,
            out_specs=[on_chip] * 9,
            scratch_shapes=scratch,
            compiler_params=pltpu.CompilerParams(collective_id=0, has_side_effects=True, vmem_limit_bytes=STEP_MIB * MIB),
            name="step",
        )(*shaped([t[0] for t in terms]), *shaped(weights), *map(stay, (*turned(m), *turned(v))))
        outs = pl.pallas_call(
            write_kernel,
            out_shape=[jax.ShapeDtypeStruct(s, BF16) for s in big] + [jax.ShapeDtypeStruct(s, F32) for s in ends * 2],
            in_specs=[on_chip] * 9,
            out_specs=[anywhere] * 9,
            scratch_shapes=[pltpu.SemaphoreType.DMA((9,))],
            compiler_params=pltpu.CompilerParams(vmem_limit_bytes=2 * MIB),
            name="write",
        )(*made)
        news = tuple(one.reshape(w.shape) for one, w in zip(outs, weights))
        return (*news, *turned(outs[3:6]), *turned(outs[6:9]))

    all_of, cut = P(None, None, None), P(None, "dp", None)
    return jax.shard_map(
        step,
        mesh=mesh,
        in_specs=(P(("rep", "dp"), None, None, None),) * 3 + (all_of,) * 3 + (cut,) * 6,
        out_specs=(P("rep", None, None),) * 3 + (P("rep", "dp", None),) * 6,
        check_vma=False,
    )
```

```python
import functools

import jax
import jax.numpy as jnp
from jax import lax
from jax.experimental import pallas as pl
from jax.experimental.pallas import tpu as pltpu
from jax.sharding import PartitionSpec as P

MESH = pl.DeviceIdType.MESH
F32, BF16 = jnp.float32, jnp.bfloat16
ROWS, PAD = 14, 16
BLOCK, TALL = 4 * ROWS, 40
STRIDE = (16, 4, 1)
X, Y, Z = GATE, UP, DOWN = range(3)
PAIR = (0, 1)
SIGN = (1, -1)
ALL = slice(None)
MIB = 1024 * 1024
STEP_MIB = 34


def place():
    me = lax.axis_index("dp")
    c = (lax.div(me, 16), lax.rem(lax.div(me, 4), 4), lax.rem(me, 4))

    def peer(axis, shift):
        return me + (lax.rem(c[axis] + (shift % 4), 4) - c[axis]) * STRIDE[axis]

    return c, peer


def mod4(value):
    return lax.rem(value + 8, 4)


def greet(peers):
    barrier = pltpu.get_barrier_semaphore()
    for p in peers:
        pl.semaphore_signal(barrier, inc=1, device_id={"dp": p}, device_id_type=MESH)
    pl.semaphore_wait(barrier, len(peers))


class Sends:
    def __init__(self, send, recv):
        self.send, self.recv, self.next = send, recv, 0

    def semaphore(self):
        self.next += 1
        return self.recv.at[self.next - 1]

    def start(self, group, src, dst, device, arrival):
        pltpu.make_async_remote_copy(
            src_ref=src, dst_ref=dst, send_sem=self.send.at[group], recv_sem=arrival, device_id={"dp": device}, device_id_type=MESH
        ).start()


def await_bytes(ref, semaphore):
    pltpu.make_async_copy(ref, ref, semaphore).wait()


class Ring:
    def __init__(self, sends, c, peer, group, axis, slot, onward, near, far):
        self.sends, self.peer, self.group, self.axis, self.slot = sends, peer, group, axis, slot
        self.k = c[axis]
        self.left, self.right = mod4(self.k - 1), mod4(self.k + 1)
        self.onward, self.near, self.far = onward, near, far

    def start(self, layer):
        here = self.slot(layer, self.k)
        self.sends.start(self.group, here, here, self.peer(self.axis, SIGN[layer]), self.onward)
        self.sends.start(self.group, here, here, self.peer(self.axis, -SIGN[layer]), self.near)

    def forward(self):
        await_bytes(self.slot(ALL, self.left), self.onward)
        for layer, k in zip(PAIR, (self.left, self.right)):
            here = self.slot(layer, k)
            self.sends.start(self.group, here, here, self.peer(self.axis, SIGN[layer]), self.far)


def step_kernel(cols, count, *refs):
    it = iter(refs)
    take = lambda n: [next(it) for _ in range(n)]
    three = lambda: take(3)
    quarter = cols // 4
    g, w, m, v = three(), three(), three(), three()
    out, new_m, new_v = three(), three(), three()
    sb2, sf2, ro2, rx2 = three(), three(), three(), three()
    sb3, sf3, ro3, rx3 = three(), three(), three(), three()
    own_m, own_v, own_w, own_g = three(), three(), three(), three()
    packed = take(2)
    fold, packs, raw_w, raw_m, raw_v, parts, send, recv, lsem, psem = take(10)
    (x, y, z), peer = place()
    c = (x, y, z)
    sends = Sends(send, recv)
    AXES = ((X, Y, Z), (Y, Z, X), (Z, X, Y))
    ro1, rd1, rs1, own1 = ([lambda layer, p, a=a, n=n: out[a].at[layer, n, p] for a in range(3)] for n in range(4))
    cases = [(a, p) for p in range(4) for a in range(3)]

    def order(axis, layer):
        s = SIGN[layer]
        return [mod4(c[axis] + d) for d in (2, -s, s, 0)]

    def block(a, layer, k, j):
        if a == GATE:
            return g[a].at[layer, k, j]
        if a == UP:
            return g[a].at[layer, j, k]
        return g[a].at[layer, j, :, k]

    UNITS = (Y, X, X)

    def unit(a, layer, k, p):
        return block(a, layer, k, order(UNITS[a], layer)[p])

    def mine(a, layer, role):
        k = order(AXES[a][0], layer)[role]
        return pltpu.make_async_copy(block(a, layer, k, ALL), out[a].at[layer, 3], lsem.at[2 * a + layer])

    def sent(a, phase):
        if phase == 0:
            ref = out[a].at[:, 0:3]
        elif phase == 1:
            ref = out[a].at[:, 0:3, :, 0] if a == DOWN else packed[a].at[:, 0:3]
        else:
            ref = out[a].at[:, 0:3, 0, 0] if a == DOWN else packed[a].at[:, 0:3, 0]
        await_bytes(ref, send.at[3 * phase + a])

    greet([peer(axis, side) for axis in (X, Y, Z) for side in SIGN])

    opp1, end1 = ({case: sends.semaphore() for case in cases} for _ in range(2))
    for a, p in cases:
        for layer in PAIR:
            ax, s = AXES[a][0], SIGN[layer]
            sends.start(a, unit(a, layer, mod4(c[ax] + 2), p), ro1[a](layer, p), peer(ax, s), opp1[a, p])
            if p == 0:
                mine(a, layer, 2).start()
    for a, p in cases:
        for layer in PAIR:
            ax, s = AXES[a][0], SIGN[layer]
            sends.start(a, unit(a, layer, mod4(c[ax] - s), p), rd1[a](layer, p), peer(ax, -s), end1[a, p])
    small = []
    for n, (src, raw, whole) in enumerate(((m, raw_m, own_m), (v, raw_v, own_v), (w, raw_w, own_w))):
        one, other = lsem.at[6 + n], lsem.at[9 + n]
        for a in (GATE, UP):
            pltpu.make_async_copy(src[a].at[:, x, y] if n == 2 else src[a], raw.at[a], one).start()
        last = pltpu.make_async_copy(src[DOWN].at[:, x, y, z] if n == 2 else src[DOWN], whole[DOWN], other)
        last.start()
        small += [pltpu.make_async_copy(raw, raw, one), last]

    def pack(rows):
        for n in range(4):
            fold[0:BLOCK, :] = rows(slice(n * quarter, (n + 1) * quarter))
            for k in range(4):
                packs[k, n * ROWS : n * ROWS + PAD, :] = fold[k * ROWS : k * ROWS + PAD, :]

    def unpack(pieces, dst):
        for k in range(4):
            packs[k, 0:BLOCK, :] = pieces[k].astype(F32)
        for n in range(4):
            for k in range(4):
                fold[k * ROWS : k * ROWS + PAD, :] = packs[k, n * ROWS : n * ROWS + PAD, :]
            dst[:, n * quarter : (n + 1) * quarter] = fold[0:BLOCK, :].astype(BF16)

    fold[BLOCK:, :] = jnp.zeros((64 - BLOCK, quarter), F32)
    packs[:, BLOCK:, :] = jnp.zeros((4, 64 - BLOCK, quarter), F32)
    for copy in small:
        copy.wait()
    for src, dst in ((raw_m, own_m), (raw_v, own_v)):
        for a in (GATE, UP):
            @pl.loop(0, ROWS)
            def _(r):
                rows = src[a, r]
                for layer in PAIR:
                    for n in range(4):
                        dst[a][layer, pl.ds(n * ROWS + r, 1), :] = rows[layer : layer + 1, n * quarter : (n + 1) * quarter]
    for a in (GATE, UP):
        for layer in PAIR:
            pack(lambda at: raw_w[a, layer, :, at].astype(F32))
            own_w[a][layer] = packs[z, 0:BLOCK, :]

    def add(dst, one, two):
        if one.shape[0] == 4:
            for k in range(4):
                dst[k] = (one[k].astype(F32) + two[k].astype(F32)).astype(BF16)
        elif one.shape[1] == cols:
            @pl.loop(0, 4)
            def _(n):
                at = pl.ds(pl.multiple_of(n * quarter, quarter), quarter)
                dst[:, at] = (one[:, at].astype(F32) + two[:, at].astype(F32)).astype(BF16)
        else:
            dst[...] = (one[...].astype(F32) + two[...].astype(F32)).astype(BF16)

    def total(refs, at):
        one, two, three = (r[at].astype(F32) for r in refs)
        return one + two + three

    for a, p in cases:
        await_bytes(out[a].at[:, 0, p], opp1[a, p])
        for layer in PAIR:
            if p == 0:
                mine(a, layer, 2).wait()
            here = ro1[a](layer, p)
            add(here, here, own1[a](layer, order(UNITS[a], layer)[p]))
            sends.start(a, here, rs1[a](layer, p), peer(AXES[a][0], SIGN[layer]), end1[a, p])
            if p == 3:
                mine(a, layer, 3).start()

    opp2, end2 = ({case: sends.semaphore() for case in cases} for _ in range(2))

    def keep2(a, layer, r2, r3, value):
        ax, s = AXES[a][1], SIGN[layer]
        if r2 >= 2:
            sf2[a][layer, r2 - 2, r3] = value
            return
        sb2[a][layer, r2, r3] = value.astype(BF16)
        here = sb2[a].at[layer, r2, r3]
        if r2 == 0:
            sends.start(3 + a, here, ro2[a].at[layer, r3], peer(ax, s), opp2[a, r3])
        else:
            sends.start(3 + a, here, rx2[a].at[layer, 0, r3], peer(ax, -s), end2[a, r3])

    for a, p in cases:
        await_bytes(out[a].at[:, 1:3, p], end1[a, p])
        for layer in PAIR:
            if p == 0:
                mine(a, layer, 3).wait()
            terms = [own1[a](layer, order(UNITS[a], layer)[p]), rs1[a](layer, p), rd1[a](layer, p)]
            pieces = order(Y if a == DOWN else Z, layer)
            if a == DOWN:
                for q, k in enumerate(pieces):
                    keep2(a, layer, p, q, total(terms, k))
                continue
            pack(lambda at: total(terms, (ALL, at)))
            for q, k in enumerate(pieces):
                r2, r3 = (q, p) if a == UP else (p, q)
                keep2(a, layer, r2, r3, packs[k, 0:BLOCK, :])

    for a, r3 in cases:
        await_bytes(ro2[a].at[:, r3], opp2[a, r3])
        for layer in PAIR:
            here = ro2[a].at[layer, r3]
            add(here, here, sf2[a].at[layer, 0, r3])
            sends.start(3 + a, here, rx2[a].at[layer, 1, r3], peer(AXES[a][1], SIGN[layer]), end2[a, r3])
    for a in range(3):
        sent(a, 0)

    opp3, end3 = ([sends.semaphore() for _ in range(3)] for _ in range(2))
    for a, r3 in cases:
        await_bytes(rx2[a].at[:, :, r3], end2[a, r3])
        for layer in PAIR:
            ax, s = AXES[a][2], SIGN[layer]
            value = total((sf2[a].at[layer, 1, r3], rx2[a].at[layer, 0, r3], rx2[a].at[layer, 1, r3]), ...)
            if r3 >= 2:
                sf3[a][layer, r3 - 2] = value
                continue
            sb3[a][layer, r3] = value.astype(BF16)
            here = sb3[a].at[layer, r3]
            if r3 == 0:
                sends.start(6 + a, here, ro3[a].at[layer], peer(ax, s), opp3[a])
            else:
                sends.start(6 + a, here, rx3[a].at[layer, 0], peer(ax, -s), end3[a])
        if r3 == 2:
            await_bytes(ro3[a], opp3[a])
            for layer in PAIR:
                here = ro3[a].at[layer]
                add(here, here, sf3[a].at[layer, 0])
                sends.start(6 + a, here, rx3[a].at[layer, 1], peer(AXES[a][2], SIGN[layer]), end3[a])

    lines = jnp.zeros((8, 128), F32)
    for a in range(3):
        await_bytes(rx3[a], end3[a])
        for layer in PAIR:
            value = total((sf3[a].at[layer, 1], rx3[a].at[layer, 0], rx3[a].at[layer, 1]), ...)
            value = value.astype(BF16).astype(F32)
            own_g[a][layer] = value
            value = value * value
            value = sum(value[r : r + 8] for r in range(0, value.shape[0], 8))
            lines += sum(value[:, k : k + 128] for k in range(0, value.shape[1], 128))

    me = lax.axis_index("dp")
    parts[me] = jnp.sum(lines, axis=0, keepdims=True)

    @pl.loop(1, 64)
    def _(n):
        pltpu.make_async_remote_copy(
            src_ref=parts.at[me], dst_ref=parts.at[me], send_sem=psem.at[0], recv_sem=psem.at[1],
            device_id={"dp": lax.rem(me + n, 64)}, device_id_type=MESH,
        ).start()
    for a in range(3):
        sent(a, 1)
        sent(a, 2)
    await_bytes(parts.at[0:63], psem.at[1])
    value = jnp.sum(parts[...], axis=0)
    squares = jnp.full((8, 128), jnp.sum(value), F32)
    factor = jnp.minimum(1.0, 0.5 * lax.rsqrt(squares / count + 1e-30))[0:1, 0:1]

    sends.next = 0

    def piece(a, i, j):
        if a == DOWN:
            return lambda layer: out[a].at[layer, i, j, z]
        return lambda layer: packed[a].at[layer, i, j]

    def slot1(a):
        if a == UP:
            return lambda layer, k: piece(a, k, z)(layer)
        return lambda layer, k: piece(a, y if a == GATE else x, k)(layer)

    def slot2(a, fixed):
        if a == UP:
            return lambda layer, k: piece(a, fixed, k)(layer)
        return lambda layer, k: piece(a, k, fixed)(layer)

    def slot3(a, fixed):
        if a == GATE:
            return lambda layer, k: out[a].at[layer, k, fixed]
        if a == UP:
            return lambda layer, k: out[a].at[layer, fixed, k]
        return lambda layer, k: out[a].at[layer, fixed, :, k]

    def near_first(axis):
        return [mod4(c[axis] + d) for d in (0, -1, 1, 2)]

    def rings(a, phase, slot, fixed, shared):
        near, far = (sends.semaphore() for _ in range(2)) if shared else (None, None)
        made = []
        for k in fixed:
            end = None if shared else sends.semaphore()
            made.append(Ring(sends, c, peer, 3 * phase + a, AXES[a][phase], slot(k), sends.semaphore(), near or end, far or end))
        return made

    first = [rings(a, 2, lambda _, a=a: slot1(a), [0], True)[0] for a in range(3)]
    second = [rings(a, 1, functools.partial(slot2, a), near_first(AXES[a][2]), a != UP) for a in range(3)]
    third = [rings(a, 0, functools.partial(slot3, a), near_first(UNITS[a]), False) for a in range(3)]

    for a in range(3):
        for layer in PAIR:
            gg = own_g[a][layer] * factor
            ww = own_w[a][layer].astype(F32)
            mm = 0.9 * own_m[a][layer] + 0.1 * gg
            vv = 0.95 * own_v[a][layer] + 0.05 * gg * gg
            here = first[a].slot(layer, c[AXES[a][2]])
            here[...] = (ww - 0.02 * (mm * lax.rsqrt(vv + 1e-8) + 0.1 * ww)).astype(BF16)
            first[a].start(layer)
            second[a][0].start(layer)
            own_m[a][layer], own_v[a][layer] = mm, vv

    def last(a, n):
        k = near_first(UNITS[a])[n]
        for layer in PAIR:
            if a != DOWN:
                unpack(packed[a].at[layer, k], third[a][n].slot(layer, c[AXES[a][0]]))
            third[a][n].start(layer)

    def near2(a):
        await_bytes(out[a].at[:, 0, :, 0] if a == DOWN else packed[a].at[:, 0], second[a][0].near)

    def far2(a):
        await_bytes(out[a].at[:, 0, :, 0] if a == DOWN else packed[a].at[:, 0], second[a][0].far)

    def up2(n):
        await_bytes(packed[UP].at[:, 0, 0:2], second[UP][n].near)

    for r in first:
        r.forward()
    for a in range(3):
        await_bytes(first[a].slot(ALL, 0), first[a].near)
        for r in second[a][1:3]:
            for layer in PAIR:
                r.start(layer)
    for a in range(3):
        await_bytes(first[a].slot(ALL, 0), first[a].far)
        for layer in PAIR:
            second[a][3].start(layer)
    for n in range(4):
        for a in (UP, GATE, DOWN):
            second[a][n].forward()
    last(DOWN, 0)
    last(GATE, 0)
    up2(0)
    last(UP, 0)
    for a in (DOWN, GATE):
        near2(a)
        last(a, 1)
        last(a, 2)
    for n in range(1, 4):
        up2(n)
        last(UP, n)
    for a in (DOWN, GATE):
        far2(a)
        last(a, 3)

    for own, new in ((own_m, new_m), (own_v, new_v)):
        new[DOWN][...] = own[DOWN][...]
        for a in (GATE, UP):
            @pl.loop(0, ROWS)
            def _(r):
                for layer in PAIR:
                    for n in range(4):
                        new[a][r, layer : layer + 1, n * quarter : (n + 1) * quarter] = own[a][layer, pl.ds(n * ROWS + r, 1), :]

    for n in range(4):
        for a in range(3):
            third[a][n].forward()
    for n in range(4):
        for a in range(3):
            await_bytes(out[a].at[:, 0, :, 0:2] if a == DOWN else out[a].at[:, 0, 0:2], third[a][n].far)
    for a in range(3):
        for phase in range(3):
            sent(a, phase)
    await_bytes(parts.at[0:63], psem.at[0])


def write_kernel(*refs):
    *refs, sem = refs
    count = len(refs) // 2
    copies = []
    for n, (src, dst) in reversed(list(enumerate(zip(refs[:count], refs[count:])))):
        copies.append(pltpu.make_async_copy(src, dst, sem.at[n]))
        copies[-1].start()
    for copy in copies:
        copy.wait()


def solution(mesh):
    def step(*arrays):
        terms, weights, m, v = (arrays[i : i + 3] for i in (0, 3, 6, 9))
        cols, fcols = terms[GATE].shape[-1], terms[DOWN].shape[-1]
        rows, frows = terms[GATE].shape[-2], terms[DOWN].shape[-2]
        assert rows == 64 * ROWS and frows == 64 * TALL and cols % 512 == 0
        wide = lambda t: t.reshape(2, 4, 4, BLOCK, cols)
        tall = lambda t: t.reshape(2, 4, 4, 4, TALL, fcols)
        shaped = lambda three: (*map(wide, three[:DOWN]), tall(three[DOWN]))
        turn = lambda t: t.transpose(1, 0, 2)
        turned = lambda three: (*map(turn, three[:DOWN]), three[DOWN])
        stay = lambda t: pltpu.with_memory_space_constraint(t, pltpu.HBM)
        count = 2 * (2 * rows * cols + frows * fcols)
        anywhere, on_chip, off_chip = (pl.BlockSpec(memory_space=space) for space in (pl.ANY, pltpu.VMEM, pltpu.HBM))
        piece = (BLOCK, cols // 4)
        pieces = (piece, piece, (TALL, fcols))
        every = lambda dtype, *lead: [pltpu.VMEM((*lead, *p), dtype) for p in pieces]
        scratch = [*every(BF16, 2, 2, 4), *every(F32, 2, 2, 4), *every(BF16, 2, 4), *every(BF16, 2, 2, 4)]
        scratch += [*every(BF16, 2, 2), *every(F32, 2, 2), *every(BF16, 2), *every(BF16, 2, 2)]
        scratch += [*every(F32, 2), *every(F32, 2), *every(F32, 2)[:DOWN], every(BF16, 2)[DOWN], *every(F32, 2)]
        scratch += every(BF16, 2, 4, 4)[:DOWN]
        scratch += [pltpu.VMEM((64, cols // 4), F32), pltpu.VMEM((4, 64, cols // 4), F32), pltpu.VMEM((2, 2, BLOCK, cols), BF16)]
        scratch += [pltpu.VMEM((2, ROWS, 2, cols), F32)] * 2 + [pltpu.VMEM((64, 1, 128), F32)]
        scratch += [pltpu.SemaphoreType.DMA((n,)) for n in (9, 54, 12, 2)]
        ends = [(ROWS, 2, cols), (ROWS, 2, cols), (2, TALL, fcols)]
        big = [(2, 4, 4, BLOCK, cols), (2, 4, 4, BLOCK, cols), (2, 4, 4, 4, TALL, fcols)]
        made = pl.pallas_call(
            functools.partial(step_kernel, cols, count),
            out_shape=[pltpu.VMEM(s, BF16) for s in big] + [pltpu.VMEM(s, F32) for s in ends * 2],
            in_specs=[off_chip] * 12,
            out_specs=[on_chip] * 9,
            scratch_shapes=scratch,
            compiler_params=pltpu.CompilerParams(collective_id=0, has_side_effects=True, vmem_limit_bytes=STEP_MIB * MIB),
            name="step",
        )(*shaped([t[0] for t in terms]), *shaped(weights), *map(stay, (*turned(m), *turned(v))))
        outs = pl.pallas_call(
            write_kernel,
            out_shape=[jax.ShapeDtypeStruct(s, BF16) for s in big] + [jax.ShapeDtypeStruct(s, F32) for s in ends * 2],
            in_specs=[on_chip] * 9,
            out_specs=[anywhere] * 9,
            scratch_shapes=[pltpu.SemaphoreType.DMA((9,))],
            compiler_params=pltpu.CompilerParams(vmem_limit_bytes=2 * MIB),
            name="write",
        )(*made)
        news = tuple(one.reshape(w.shape) for one, w in zip(outs, weights))
        return (*news, *turned(outs[3:6]), *turned(outs[6:9]))

    all_of, cut = P(None, None, None), P(None, "dp", None)
    return jax.shard_map(
        step,
        mesh=mesh,
        in_specs=(P(("rep", "dp"), None, None, None),) * 3 + (all_of,) * 3 + (cut,) * 6,
        out_specs=(P("rep", None, None),) * 3 + (P("rep", "dp", None),) * 6,
        check_vma=False,
    )
```

```python
import functools

import jax
import jax.numpy as jnp
from jax import lax
from jax.experimental import pallas as pl
from jax.experimental.pallas import tpu as pltpu
from jax.sharding import PartitionSpec as P

MESH = pl.DeviceIdType.MESH
F32, BF16 = jnp.float32, jnp.bfloat16
ROWS, PAD = 14, 16
BLOCK, TALL = 4 * ROWS, 40
STRIDE = (16, 4, 1)
X, Y, Z = GATE, UP, DOWN = range(3)
PAIR = (0, 1)
SIGN = (1, -1)
ALL = slice(None)
MIB = 1024 * 1024
STEP_MIB = 34
LATE = 1


def place():
    me = lax.axis_index("dp")
    c = (lax.div(me, 16), lax.rem(lax.div(me, 4), 4), lax.rem(me, 4))

    def peer(axis, shift):
        return me + (lax.rem(c[axis] + (shift % 4), 4) - c[axis]) * STRIDE[axis]

    return c, peer


def mod4(value):
    return lax.rem(value + 8, 4)


def greet(peers):
    barrier = pltpu.get_barrier_semaphore()
    for p in peers:
        pl.semaphore_signal(barrier, inc=1, device_id={"dp": p}, device_id_type=MESH)
    pl.semaphore_wait(barrier, len(peers))


class Sends:
    def __init__(self, send, recv):
        self.send, self.recv, self.next = send, recv, 0

    def semaphore(self):
        self.next += 1
        return self.recv.at[self.next - 1]

    def start(self, group, src, dst, device, arrival):
        pltpu.make_async_remote_copy(
            src_ref=src, dst_ref=dst, send_sem=self.send.at[group], recv_sem=arrival, device_id={"dp": device}, device_id_type=MESH
        ).start()


def await_bytes(ref, semaphore):
    pltpu.make_async_copy(ref, ref, semaphore).wait()


class Ring:
    def __init__(self, sends, c, peer, group, axis, slot, onward, near, far):
        self.sends, self.peer, self.group, self.axis, self.slot = sends, peer, group, axis, slot
        self.k = c[axis]
        self.left, self.right = mod4(self.k - 1), mod4(self.k + 1)
        self.onward, self.near, self.far = onward, near, far

    def start(self, layer):
        here = self.slot(layer, self.k)
        self.sends.start(self.group, here, here, self.peer(self.axis, SIGN[layer]), self.onward)
        self.sends.start(self.group, here, here, self.peer(self.axis, -SIGN[layer]), self.near)

    def forward(self):
        await_bytes(self.slot(ALL, self.left), self.onward)
        for layer, k in zip(PAIR, (self.left, self.right)):
            here = self.slot(layer, k)
            self.sends.start(self.group if self.group >= 3 else 9 + self.group, here, here, self.peer(self.axis, SIGN[layer]), self.far)


def step_kernel(cols, count, *refs):
    it = iter(refs)
    take = lambda n: [next(it) for _ in range(n)]
    three = lambda: take(3)
    quarter = cols // 4
    g, w, m, v = three(), three(), three(), three()
    out, new_m, new_v, on = three(), three(), three(), (three(), three())
    sb2, sf2, ro2, rx2 = three(), three(), three(), three()
    sb3, sf3, ro3, rx3 = three(), three(), three(), three()
    own_m, own_v, own_w, own_g = three(), three(), three(), three()
    packed = take(2)
    fold, packs, raw_w, raw_m, raw_v, parts, send, recv, lsem, psem = take(10)
    (x, y, z), peer = place()
    c = (x, y, z)
    sends = Sends(send, recv)
    AXES = ((X, Y, Z), (Y, Z, X), (Z, X, Y))
    ro1, rd1, rs1, own1 = ([lambda layer, p, a=a, n=n: out[a].at[layer, n, p] for a in range(3)] for n in range(4))
    cases = [(a, p) for p in range(4) for a in range(3)]

    def order(axis, layer):
        s = SIGN[layer]
        return [mod4(c[axis] + d) for d in (2, -s, s, 0)]

    def block(a, layer, k, j):
        if a == GATE:
            return g[a].at[layer, k, j]
        if a == UP:
            return g[a].at[layer, j, k]
        return g[a].at[layer, j, :, k]

    UNITS = (Y, X, X)

    def unit(a, layer, k, p):
        return block(a, layer, k, order(UNITS[a], layer)[p])

    def mine(a, layer, role):
        k = order(AXES[a][0], layer)[role]
        return pltpu.make_async_copy(block(a, layer, k, ALL), out[a].at[layer, 3], lsem.at[2 * a + layer])

    def sent(a, phase):
        if phase == 0:
            ref = out[a].at[:, 0:3]
        elif phase == 1:
            ref = out[a].at[:, 0:3, :, 0] if a == DOWN else packed[a].at[:, 0:3]
        else:
            ref = out[a].at[:, 0:3, 0, 0] if a == DOWN else packed[a].at[:, 0:3, 0]
        await_bytes(ref, send.at[3 * phase + a])

    greet([peer(axis, side) for axis in (X, Y, Z) for side in SIGN])

    opp1, end1 = ({case: sends.semaphore() for case in cases} for _ in range(2))
    for a, p in cases:
        for layer in PAIR:
            ax, s = AXES[a][0], SIGN[layer]
            sends.start(a, unit(a, layer, mod4(c[ax] + 2), p), ro1[a](layer, p), peer(ax, s), opp1[a, p])
            if p == 0:
                mine(a, layer, 2).start()
    for a, p in cases:
        for layer in PAIR:
            ax, s = AXES[a][0], SIGN[layer]
            sends.start(a, unit(a, layer, mod4(c[ax] - s), p), rd1[a](layer, p), peer(ax, -s), end1[a, p])
    small = []
    for n, (src, raw, whole) in enumerate(((m, raw_m, own_m), (v, raw_v, own_v), (w, raw_w, own_w))):
        one, other = lsem.at[6 + n], lsem.at[9 + n]
        for a in (GATE, UP):
            pltpu.make_async_copy(src[a].at[:, x, y] if n == 2 else src[a], raw.at[a], one).start()
        last = pltpu.make_async_copy(src[DOWN].at[:, x, y, z] if n == 2 else src[DOWN], whole[DOWN], other)
        last.start()
        small += [pltpu.make_async_copy(raw, raw, one), last]

    def pack(rows):
        for n in range(4):
            fold[0:BLOCK, :] = rows(slice(n * quarter, (n + 1) * quarter))
            for k in range(4):
                packs[k, n * ROWS : n * ROWS + PAD, :] = fold[k * ROWS : k * ROWS + PAD, :]

    def unpack(pieces, dst):
        for k in range(4):
            packs[k, 0:BLOCK, :] = pieces[k].astype(F32)
        for n in range(4):
            for k in range(4):
                fold[k * ROWS : k * ROWS + PAD, :] = packs[k, n * ROWS : n * ROWS + PAD, :]
            dst[:, n * quarter : (n + 1) * quarter] = fold[0:BLOCK, :].astype(BF16)

    fold[BLOCK:, :] = jnp.zeros((64 - BLOCK, quarter), F32)
    packs[:, BLOCK:, :] = jnp.zeros((4, 64 - BLOCK, quarter), F32)
    for copy in small:
        copy.wait()
    for src, dst in ((raw_m, own_m), (raw_v, own_v)):
        for a in (GATE, UP):
            @pl.loop(0, ROWS)
            def _(r):
                rows = src[a, r]
                for layer in PAIR:
                    for n in range(4):
                        dst[a][layer, pl.ds(n * ROWS + r, 1), :] = rows[layer : layer + 1, n * quarter : (n + 1) * quarter]
    for a in (GATE, UP):
        for layer in PAIR:
            pack(lambda at: raw_w[a, layer, :, at].astype(F32))
            own_w[a][layer] = packs[z, 0:BLOCK, :]

    def add(dst, one, two):
        if one.shape[0] == 4:
            for k in range(4):
                dst[k] = (one[k].astype(F32) + two[k].astype(F32)).astype(BF16)
        elif one.shape[1] == cols:
            @pl.loop(0, 4)
            def _(n):
                at = pl.ds(pl.multiple_of(n * quarter, quarter), quarter)
                dst[:, at] = (one[:, at].astype(F32) + two[:, at].astype(F32)).astype(BF16)
        else:
            dst[...] = (one[...].astype(F32) + two[...].astype(F32)).astype(BF16)

    def total(refs, at):
        one, two, three = (r[at].astype(F32) for r in refs)
        return one + two + three

    for a, p in cases:
        await_bytes(out[a].at[:, 0, p], opp1[a, p])
        for layer in PAIR:
            if p == 0:
                mine(a, layer, 2).wait()
            here = ro1[a](layer, p)
            add(here, here, own1[a](layer, order(UNITS[a], layer)[p]))
            sends.start(a, here, rs1[a](layer, p), peer(AXES[a][0], SIGN[layer]), end1[a, p])
            if p == 3:
                mine(a, layer, 3).start()

    opp2, end2 = ({case: sends.semaphore() for case in cases} for _ in range(2))

    def keep2(a, layer, r2, r3, value):
        ax, s = AXES[a][1], SIGN[layer]
        if r2 >= 2:
            sf2[a][layer, r2 - 2, r3] = value
            return
        sb2[a][layer, r2, r3] = value.astype(BF16)
        here = sb2[a].at[layer, r2, r3]
        if r2 == 0:
            sends.start(3 + a, here, ro2[a].at[layer, r3], peer(ax, s), opp2[a, r3])
        else:
            sends.start(3 + a, here, rx2[a].at[layer, 0, r3], peer(ax, -s), end2[a, r3])

    for a, p in cases:
        await_bytes(out[a].at[:, 1:3, p], end1[a, p])
        for layer in PAIR:
            if p == 0:
                mine(a, layer, 3).wait()
            terms = [own1[a](layer, order(UNITS[a], layer)[p]), rs1[a](layer, p), rd1[a](layer, p)]
            pieces = order(Y if a == DOWN else Z, layer)
            if a == DOWN:
                for q, k in enumerate(pieces):
                    keep2(a, layer, p, q, total(terms, k))
                continue
            pack(lambda at: total(terms, (ALL, at)))
            for q, k in enumerate(pieces):
                r2, r3 = (q, p) if a == UP else (p, q)
                keep2(a, layer, r2, r3, packs[k, 0:BLOCK, :])

    for a, r3 in cases:
        await_bytes(ro2[a].at[:, r3], opp2[a, r3])
        for layer in PAIR:
            here = ro2[a].at[layer, r3]
            add(here, here, sf2[a].at[layer, 0, r3])
            sends.start(3 + a, here, rx2[a].at[layer, 1, r3], peer(AXES[a][1], SIGN[layer]), end2[a, r3])
    for a in range(3):
        sent(a, 0)

    opp3, end3 = ([sends.semaphore() for _ in range(3)] for _ in range(2))
    for a, r3 in cases:
        await_bytes(rx2[a].at[:, :, r3], end2[a, r3])
        for layer in PAIR:
            ax, s = AXES[a][2], SIGN[layer]
            value = total((sf2[a].at[layer, 1, r3], rx2[a].at[layer, 0, r3], rx2[a].at[layer, 1, r3]), ...)
            if r3 >= 2:
                sf3[a][layer, r3 - 2] = value
                continue
            sb3[a][layer, r3] = value.astype(BF16)
            here = sb3[a].at[layer, r3]
            if r3 == 0:
                sends.start(6 + a, here, ro3[a].at[layer], peer(ax, s), opp3[a])
            else:
                sends.start(6 + a, here, rx3[a].at[layer, 0], peer(ax, -s), end3[a])
        if r3 == 2:
            await_bytes(ro3[a], opp3[a])
            for layer in PAIR:
                here = ro3[a].at[layer]
                add(here, here, sf3[a].at[layer, 0])
                sends.start(6 + a, here, rx3[a].at[layer, 1], peer(AXES[a][2], SIGN[layer]), end3[a])

    lines = jnp.zeros((8, 128), F32)
    for a in range(3):
        await_bytes(rx3[a], end3[a])
        for layer in PAIR:
            value = total((sf3[a].at[layer, 1], rx3[a].at[layer, 0], rx3[a].at[layer, 1]), ...)
            value = value.astype(BF16).astype(F32)
            own_g[a][layer] = value
            value = value * value
            value = sum(value[r : r + 8] for r in range(0, value.shape[0], 8))
            lines += sum(value[:, k : k + 128] for k in range(0, value.shape[1], 128))

    me = lax.axis_index("dp")
    parts[me] = jnp.sum(lines, axis=0, keepdims=True)
    dist = (0, 1, 2, 1)
    shifts = sorted(((i, j, k) for i in range(4) for j in range(4) for k in range(4)), key=lambda t: -sum(dist[n] for n in t))[:-1]
    px, py, pz = ([mod4(c[axis] + d) * STRIDE[axis] for d in range(4)] for axis in (X, Y, Z))
    for i, j, k in shifts:
        pltpu.make_async_remote_copy(
            src_ref=parts.at[me], dst_ref=parts.at[me], send_sem=psem.at[0], recv_sem=psem.at[1],
            device_id={"dp": px[i] + py[j] + pz[k]}, device_id_type=MESH,
        ).start()
    for a in range(3):
        sent(a, 1)
        sent(a, 2)
    await_bytes(parts.at[0:63], psem.at[1])
    value = jnp.sum(parts[...], axis=0)
    squares = jnp.full((8, 128), jnp.sum(value), F32)
    factor = jnp.minimum(1.0, 0.5 * lax.rsqrt(squares / count + 1e-30))[0:1, 0:1]

    sends.next = 0

    def piece(a, i, j):
        if a == DOWN:
            return lambda layer: out[a].at[layer, i, j, z]
        return lambda layer: packed[a].at[layer, i, j]

    def slot1(a):
        if a == UP:
            return lambda layer, k: piece(a, k, z)(layer)
        return lambda layer, k: piece(a, y if a == GATE else x, k)(layer)

    def slot2(a, fixed):
        if a == UP:
            return lambda layer, k: piece(a, fixed, k)(layer)
        return lambda layer, k: piece(a, k, fixed)(layer)

    def slot3(a, fixed):
        if a == GATE:
            return lambda layer, k: out[a].at[layer, k, fixed]
        if a == UP:
            return lambda layer, k: out[a].at[layer, fixed, k]
        return lambda layer, k: out[a].at[layer, fixed, :, k]

    def near_first(axis):
        return [mod4(c[axis] + d) for d in (0, -1, 1, 2)]

    def rings(a, phase, slot, fixed, shared):
        near, far = (sends.semaphore() for _ in range(2)) if shared else (None, None)
        made = []
        for k in fixed:
            end = None if shared else sends.semaphore()
            made.append(Ring(sends, c, peer, 3 * phase + a, AXES[a][phase], slot(k), sends.semaphore(), near or end, far or end))
        return made

    first = [rings(a, 2, lambda _, a=a: slot1(a), [0], True)[0] for a in range(3)]
    second = [rings(a, 1, functools.partial(slot2, a), near_first(AXES[a][2]), a != UP) for a in range(3)]
    third = [rings(a, 0, functools.partial(slot3, a), near_first(UNITS[a]), False) for a in range(3)]

    for a in range(3):
        for layer in PAIR:
            gg = own_g[a][layer] * factor
            ww = own_w[a][layer].astype(F32)
            mm = 0.9 * own_m[a][layer] + 0.1 * gg
            vv = 0.95 * own_v[a][layer] + 0.05 * gg * gg
            here = first[a].slot(layer, c[AXES[a][2]])
            here[...] = (ww - 0.02 * (mm * lax.rsqrt(vv + 1e-8) + 0.1 * ww)).astype(BF16)
            first[a].start(layer)
            second[a][0].start(layer)
            own_m[a][layer], own_v[a][layer] = mm, vv

    def last(a, n):
        k = near_first(UNITS[a])[n]
        for layer in PAIR:
            if a != DOWN:
                unpack(packed[a].at[layer, k], third[a][n].slot(layer, c[AXES[a][0]]))
            third[a][n].start(layer)

    def near2(a):
        await_bytes(out[a].at[:, 0, :, 0] if a == DOWN else packed[a].at[:, 0], second[a][0].near)

    def far2(a):
        await_bytes(out[a].at[:, 0, :, 0] if a == DOWN else packed[a].at[:, 0], second[a][0].far)

    def up2(n):
        await_bytes(packed[UP].at[:, 0, 0:2], second[UP][n].near)

    for r in first:
        r.forward()
    for a in range(3):
        await_bytes(first[a].slot(ALL, 0), first[a].near)
        for r in second[a][1:3]:
            for layer in PAIR:
                r.start(layer)
    for a in range(3):
        await_bytes(first[a].slot(ALL, 0), first[a].far)
        for layer in PAIR:
            second[a][3].start(layer)
    for n in range(4):
        for a in (UP, GATE, DOWN):
            second[a][n].forward()
    last(DOWN, 0)
    last(GATE, 0)
    up2(0)
    last(UP, 0)
    for a in (DOWN, GATE):
        near2(a)
        last(a, 1)
        last(a, 2)
    for n in range(1, 4):
        up2(n)
        last(UP, n)
    for a in (DOWN, GATE):
        far2(a)
        last(a, 3)

    for own, new in ((own_m, new_m), (own_v, new_v)):
        new[DOWN][...] = own[DOWN][...]
        for a in (GATE, UP):
            @pl.loop(0, ROWS)
            def _(r):
                for layer in PAIR:
                    for n in range(4):
                        new[a][r, layer : layer + 1, n * quarter : (n + 1) * quarter] = own[a][layer, pl.ds(n * ROWS + r, 1), :]

    for n in range(LATE):
        for a in range(3):
            third[a][n].forward()
    for n in range(4):
        for a in range(3):
            if n >= LATE:
                await_bytes(third[a][n].slot(ALL, 0), third[a][n].onward)
                await_bytes(third[a][n].slot(ALL, 0), third[a][n].near)
                for layer, k in zip(PAIR, (third[a][n].left, third[a][n].right)):
                    pltpu.make_async_copy(third[a][n].slot(layer, k), on[layer][a].at[n - LATE], lsem.at[2 * a + layer]).start()
                continue
            await_bytes(out[a].at[:, 0, :, 0:2] if a == DOWN else out[a].at[:, 0, 0:2], third[a][n].far)
    for a in range(3):
        sent(a, 1)
        sent(a, 2)
        await_bytes(out[a].at[:, 0:2], send.at[a])
        await_bytes(out[a].at[:, 0:LATE, 0], send.at[9 + a])
        for layer in PAIR:
            await_bytes(on[layer][a], lsem.at[2 * a + layer])
    await_bytes(parts.at[0:63], psem.at[0])


def late_blocks(c):
    AXES, UNITS = (X, Y, Z), (Y, X, X)
    for a in range(3):
        for n, d in zip(range(4 - LATE), (-1, 1, 2)[LATE - 1 :]):
            fixed = mod4(c[UNITS[a]] + d)
            if a == GATE:
                yield a, n, AXES[a], lambda ref, layer, k, fixed=fixed: ref.at[layer, k, fixed]
            elif a == UP:
                yield a, n, AXES[a], lambda ref, layer, k, fixed=fixed: ref.at[layer, fixed, k]
            else:
                yield a, n, AXES[a], lambda ref, layer, k, fixed=fixed: ref.at[layer, fixed, :, k]


def write_kernel(*refs):
    *refs, sem = refs
    count = len(refs) // 2
    copies = [pltpu.make_async_copy(src, dst, sem.at[n]) for n, (src, dst) in enumerate(zip(refs[:count], refs[count:]))]
    for copy in copies:
        copy.start()
    for copy in copies:
        copy.wait()


def late_kernel(*refs):
    far, outs, sem = (refs[3:6], refs[6:9]), refs[9:12], refs[12]
    c, _ = place()
    copies = []
    for a, n, axis, slot in late_blocks(c):
        for layer in PAIR:
            copies.append(pltpu.make_async_copy(far[layer][a].at[n], slot(outs[a], layer, mod4(c[axis] + 2)), sem.at[len(copies)]))
            copies[-1].start()
    for copy in copies:
        copy.wait()


def solution(mesh):
    def step(*arrays):
        terms, weights, m, v = (arrays[i : i + 3] for i in (0, 3, 6, 9))
        cols, fcols = terms[GATE].shape[-1], terms[DOWN].shape[-1]
        rows, frows = terms[GATE].shape[-2], terms[DOWN].shape[-2]
        assert rows == 64 * ROWS and frows == 64 * TALL and cols % 512 == 0
        wide = lambda t: t.reshape(2, 4, 4, BLOCK, cols)
        tall = lambda t: t.reshape(2, 4, 4, 4, TALL, fcols)
        shaped = lambda three: (*map(wide, three[:DOWN]), tall(three[DOWN]))
        turn = lambda t: t.transpose(1, 0, 2)
        turned = lambda three: (*map(turn, three[:DOWN]), three[DOWN])
        stay = lambda t: pltpu.with_memory_space_constraint(t, pltpu.HBM)
        count = 2 * (2 * rows * cols + frows * fcols)
        anywhere, on_chip, off_chip = (pl.BlockSpec(memory_space=space) for space in (pl.ANY, pltpu.VMEM, pltpu.HBM))
        piece = (BLOCK, cols // 4)
        pieces = (piece, piece, (TALL, fcols))
        every = lambda dtype, *lead: [pltpu.VMEM((*lead, *p), dtype) for p in pieces]
        scratch = [*every(BF16, 2, 2, 4), *every(F32, 2, 2, 4), *every(BF16, 2, 4), *every(BF16, 2, 2, 4)]
        scratch += [*every(BF16, 2, 2), *every(F32, 2, 2), *every(BF16, 2), *every(BF16, 2, 2)]
        scratch += [*every(F32, 2), *every(F32, 2), *every(F32, 2)[:DOWN], every(BF16, 2)[DOWN], *every(F32, 2)]
        scratch += every(BF16, 2, 4, 4)[:DOWN]
        scratch += [pltpu.VMEM((64, cols // 4), F32), pltpu.VMEM((4, 64, cols // 4), F32), pltpu.VMEM((2, 2, BLOCK, cols), BF16)]
        scratch += [pltpu.VMEM((2, ROWS, 2, cols), F32)] * 2 + [pltpu.VMEM((64, 1, 128), F32)]
        scratch += [pltpu.SemaphoreType.DMA((n,)) for n in (12, 54, 12, 2)]
        ends = [(ROWS, 2, cols), (ROWS, 2, cols), (2, TALL, fcols)]
        big = [(2, 4, 4, BLOCK, cols), (2, 4, 4, BLOCK, cols), (2, 4, 4, 4, TALL, fcols)]
        units = [(4 - LATE, BLOCK, cols), (4 - LATE, BLOCK, cols), (4 - LATE, 4, TALL, fcols)]
        made = pl.pallas_call(
            functools.partial(step_kernel, cols, count),
            out_shape=[pltpu.VMEM(s, BF16) for s in big] + [pltpu.VMEM(s, F32) for s in ends * 2] + [jax.ShapeDtypeStruct(s, BF16) for s in units * 2],
            in_specs=[off_chip] * 12,
            out_specs=[on_chip] * 9 + [anywhere] * 6,
            scratch_shapes=scratch,
            compiler_params=pltpu.CompilerParams(collective_id=0, has_side_effects=True, vmem_limit_bytes=STEP_MIB * MIB),
            name="step",
        )(*shaped([t[0] for t in terms]), *shaped(weights), *map(stay, (*turned(m), *turned(v))))
        far = []
        for n, block in enumerate(made[9:]):
            layer, a = divmod(n, 3)
            step_of = STRIDE[a]
            ring = [(d, d + ((d // step_of + SIGN[layer]) % 4 - d // step_of % 4) * step_of) for d in range(64)]
            far.append(lax.ppermute(block, "dp", ring))
        outs = pl.pallas_call(
            write_kernel,
            out_shape=[jax.ShapeDtypeStruct(s, BF16) for s in big] + [jax.ShapeDtypeStruct(s, F32) for s in ends * 2],
            in_specs=[on_chip] * 9,
            out_specs=[anywhere] * 9,
            scratch_shapes=[pltpu.SemaphoreType.DMA((9,))],
            compiler_params=pltpu.CompilerParams(vmem_limit_bytes=2 * MIB),
            cost_estimate=pl.CostEstimate(flops=10**8, bytes_accessed=MIB, transcendentals=0),
            name="write",
        )(*made[:9])
        ahead = outs[:3]
        outs = pl.pallas_call(
            late_kernel,
            out_shape=[jax.ShapeDtypeStruct(s, BF16) for s in big],
            in_specs=[anywhere] * 3 + [on_chip] * 6,
            out_specs=[anywhere] * 3,
            input_output_aliases={n: n for n in range(3)},
            scratch_shapes=[pltpu.SemaphoreType.DMA((18,))],
            compiler_params=pltpu.CompilerParams(vmem_limit_bytes=8 * MIB),
            name="late",
        )(*ahead, *far) + tuple(outs[3:])
        news = tuple(one.reshape(w.shape) for one, w in zip(outs, weights))
        return (*news, *turned(outs[3:6]), *turned(outs[6:9]))

    all_of, cut = P(None, None, None), P(None, "dp", None)
    return jax.shard_map(
        step,
        mesh=mesh,
        in_specs=(P(("rep", "dp"), None, None, None),) * 3 + (all_of,) * 3 + (cut,) * 6,
        out_specs=(P("rep", None, None),) * 3 + (P("rep", "dp", None),) * 6,
        check_vma=False,
    )
```
